32 devices in a mesh: ep: 8 (over z, x), etp: 4 (over y, core).
Axes of the slice: x: 2, y: 2, z: 4, core: 2. Of those that a mesh axis runs over, the one named last changes fastest.
Arguments:
- tokens: bfloat16 [1024, 4096], P('ep', 'etp'), may hold values from -6 to 6
- expert_ids: int32 [1024, 8], P('ep'), may hold values from 0 to 15, all different within a row; in each aligned block of 128 rows (0 to 127, 128 to 255, ...) at most 96 rows name the same one
- gate_prob: float32 [1024, 8], P('ep'), may hold values from 0.05 to 1
- gate_weight: bfloat16 [16, 4096, 1536], P('ep', None, 'etp'), may hold values from -0.09375 to 0.09375
- up_weight: bfloat16 [16, 4096, 1536], P('ep', None, 'etp'), may hold values from -0.09375 to 0.09375
- down_weight: bfloat16 [16, 1536, 4096], P('ep', 'etp'), may hold values from -0.15625 to 0.15625
Outputs:
- mixed: bfloat16 [1024, 4096], P('ep', 'etp')
The draws below stay inside these ranges and needn't reach their ends.
Inputs may be any that keep to these rules, and one draw needn't show every extreme that they name: `expert_ids`: each row names 8 different experts. Within each aligned block of 128 rows (one token group) no expert is named more than 96 times, and in every draw some expert is named exactly 96 times in some block.
All inputs are finite; a program needn't handle non-finite values.
Results may differ from the reference program's by a relative error of at most 0.012.
Values may be sent and summed in bfloat16 or wider, within the bound.
A program may use at most 128 MiB of HBM per device.

```python
import math
import jax
import jax.numpy as jnp
import numpy as np
from jax import lax

D = 4096
FF = 1536
TOP = 8
TOK_DEV = 128
EXPERTS = 16
GROUPS = 8
TOKENS = 1024
CAP = 96
N_ETP = 4


def shard_levels(rng, shape, split, least, top_value):
    level, own = 1.0, jax.random.fold_in(rng, 6)
    for dim, shards_of in split:
        draws = jnp.exp(jax.random.uniform(jax.random.fold_in(own, dim), (shards_of,), jnp.float32, least / len(split), top_value / len(split)))
        level = level * jnp.repeat(draws, shape[dim] // shards_of).reshape([-1 if axis == dim else 1 for axis in range(len(shape))])
    return level


def assign_block(stream_key, own, number, rows, count, top, most, lean):
    ranking = jax.random.permutation(stream_key, count)
    packed, ordinary = load_shares(count, rows * top, most, lean, True), load_shares(count, rows * top, most, lean, False)
    places = jnp.arange(count)

    def named(lengths, offset_by):
        used = int((lengths > 0).sum())
        fixed = max(1, used // 4)
        moved = fixed + (places - fixed + offset_by * (used - fixed)) % max(1, count - fixed)
        return jnp.zeros((count,), jnp.int32).at[ranking[jnp.where(places < fixed, places, moved)]].set(jnp.asarray(lengths, jnp.int32))

    lengths = jnp.where(number % 4 == 0, named(packed, number // 4), named(ordinary, number - number // 4 - 1))
    mixed = jax.random.permutation(jax.random.fold_in(own, 3), count)
    source_of, sink = mixed[0:count // 2 * 2:2], mixed[1:count // 2 * 2:2]
    slack = jnp.minimum(lengths[source_of] - 1, most - lengths[sink]) // 2
    slack = jnp.where((source_of == ranking[0]) | (sink == ranking[0]) | (lengths[sink] == 0), 0, jnp.maximum(slack, 0))
    moved = jax.random.randint(jax.random.fold_in(own, 4), (count // 2,), 0, 1 << 20) % (slack + 1)
    lengths = lengths.at[source_of].add(-moved).at[sink].add(moved)
    items = jnp.searchsorted(jnp.cumsum(lengths), jnp.arange(rows * top), side="right").astype(jnp.int32)
    grid = items.reshape(top, rows).T
    grid = grid[jax.random.permutation(jax.random.fold_in(own, 1), rows)]
    offset_by = jax.random.randint(jax.random.fold_in(own, 2), (rows, 1), 0, top)
    return jnp.take_along_axis(grid, (jnp.arange(top)[None, :] + offset_by) % top, axis=1)


def load_shares(amount, total, limit, slope, full):
    weights = [(1 << 20) // math.isqrt(standing ** slope) + 1 for standing in range(1, amount + 1)]
    largest = limit if full else min(limit, max(-(-total // amount), total * weights[0] // sum(weights)))
    least = 1 if total - largest >= amount - 1 else 0
    given, rest = [largest] + [least] * (amount - 1), total - largest - least * (amount - 1)
    while rest > 0:
        free = [i for i in range(1, amount) if given[i] < largest] or [i for i in range(1, amount) if given[i] < limit]
        whole, remaining = sum([weights[i] for i in free]), rest
        for i in free:
            more = min(limit - given[i], max(1, remaining * weights[i] // whole), rest)
            given[i] = given[i] + more
            rest = rest - more
    return np.array(given)


def scatter_about(own_key, dims, spread, most, pieces=(), kind=jnp.bfloat16):
    result = jax.random.normal(own_key, dims, jnp.float32) * spread
    if len(pieces) > 0:
        result = shard_levels(own_key, dims, pieces, -0.22, 0.18) * result
    return jnp.clip(result, min=-most, max=most).astype(kind)


def setup_inputs(seed: int = 0) -> dict:
    splits = jax.random.split(jax.random.key(seed), 7)
    tokens = scatter_about(splits[0], (TOKENS, D), 1.0, 6.0, ((0, 8), (1, 4)))
    expert_ids_keys = jax.random.split(jax.random.fold_in(splits[1], 1), TOKENS // TOK_DEV)
    expert_ids_turns = jax.random.permutation(jax.random.fold_in(splits[1], 3), TOKENS // TOK_DEV)
    expert_ids = jax.vmap(lambda own, number: assign_block(jax.random.fold_in(splits[1], 2), own, number, TOK_DEV, EXPERTS, TOP, CAP, 2))(expert_ids_keys, expert_ids_turns).reshape((TOKENS, TOP))
    gate_prob = jnp.clip(0.05 + 0.95 * jax.random.uniform(splits[2], (TOKENS, TOP), jnp.float32) ** shard_levels(splits[2], (TOKENS, TOP), ((0, 8),), -0.2, 0.2), 0.05, 1.0)
    gate_weight = scatter_about(splits[3], (EXPERTS, D, FF), D ** -0.5, 0.09375, ((0, 8), (2, 4)))
    up_weight = scatter_about(splits[4], (EXPERTS, D, FF), D ** -0.5, 0.09375, ((0, 8), (2, 4)))
    down_weight = scatter_about(splits[5], (EXPERTS, FF, D), FF ** -0.5, 0.15625, ((0, 8), (1, 4)))
    return dict(tokens=tokens, expert_ids=expert_ids, gate_prob=gate_prob, gate_weight=gate_weight, up_weight=up_weight, down_weight=down_weight)


def reference(tokens, expert_ids, gate_prob, gate_weight, up_weight, down_weight):
    assigned = TOK_DEV * TOP
    grouped = expert_ids.reshape(GROUPS, assigned).astype(jnp.int32)
    onehot = (grouped[:, :, None] == jnp.arange(EXPERTS, dtype=jnp.int32)[None, None, :]).astype(jnp.int32)
    position = jnp.sum((jnp.cumsum(onehot, axis=1) - onehot) * onehot, axis=2).astype(jnp.int32)
    slot_index = (grouped * CAP + position).astype(jnp.int32)
    group_rows = jnp.arange(GROUPS, dtype=jnp.int32)[:, None]
    owners = (group_rows * TOK_DEV + (jnp.arange(assigned, dtype=jnp.int32) // TOP)[None, :]).astype(jnp.int32)
    sources = jnp.full((GROUPS, EXPERTS * CAP), TOKENS, jnp.int32).at[group_rows, slot_index].set(owners)
    scales = jnp.zeros((GROUPS, EXPERTS * CAP), jnp.float32).at[group_rows, slot_index].set(
        gate_prob.reshape(GROUPS, assigned).astype(jnp.float32))
    sources = sources.reshape(GROUPS, EXPERTS, CAP).transpose(1, 0, 2).reshape(EXPERTS, GROUPS * CAP)
    scales = scales.reshape(GROUPS, EXPERTS, CAP).transpose(1, 0, 2).reshape(EXPERTS, GROUPS * CAP)
    padded = jnp.concatenate([tokens, jnp.zeros((1, D), tokens.dtype)], axis=0)
    block = FF // N_ETP

    def expert_step(accumulated, inputs):
        w_gate, w_up, w_down, rows_from, row_scale = inputs
        expert_rows = padded[rows_from]
        gate_sum = jnp.dot(expert_rows, w_gate, preferred_element_type=jnp.float32)
        up_sum = jnp.dot(expert_rows, w_up, preferred_element_type=jnp.float32)
        hidden = (jax.nn.silu(gate_sum) * up_sum).astype(jnp.bfloat16)
        expert_out = jnp.zeros((GROUPS * CAP, D), jnp.float32)
        for part_index in range(N_ETP):
            product = jnp.dot(hidden[:, part_index * block:(part_index + 1) * block],
                              w_down[part_index * block:(part_index + 1) * block, :],
                              preferred_element_type=jnp.float32)
            rounded = lax.optimization_barrier(product.astype(jnp.bfloat16))
            expert_out = expert_out + rounded.astype(jnp.float32)
        accumulated = accumulated.at[rows_from].add(row_scale[:, None] * expert_out)
        return accumulated, None

    accumulated = jnp.zeros((TOKENS + 1, D), jnp.float32)
    accumulated, unused = lax.scan(expert_step, accumulated,
                                   (gate_weight, up_weight, down_weight, sources, scales))
    return accumulated[:TOKENS].astype(jnp.bfloat16)
```

```python
import functools
import math

import jax
import jax.numpy as jnp
from jax import lax
from jax.experimental import pallas as pl
from jax.experimental.pallas import tpu as pltpu
from jax.sharding import PartitionSpec as P

MESH = pl.DeviceIdType.MESH
VMEM_BUDGET = 56 << 20


def place(sizes):
    ep, etp = lax.axis_index("ep"), lax.axis_index("etp")
    return (ep // 2, ep % 2, etp // 2, etp % 2)


def flip(at, bits):
    bit = 1
    while bit <= bits:
        if bits & bit:
            at = at + bit - 2 * bit * ((at // bit) % 2)
        bit *= 2
    return at


def moved(here, sizes, rel):
    return tuple(flip(h, r) for h, r in zip(here, rel))


def device(at):
    z, x, y, c = at
    return (z * 2 + x, y * 2 + c)


def layer_kernel(sizes, x_hbm, ids_hbm, prob_hbm, gate_hbm, up_hbm, down_hbm, out_ref,
                 x_ref, ids_ref, prob_ref, own_share, share_ref, w_ref, down_ref, hid_ref, part_ref,
                 buf_c, buf_1, buf_2, buf_z,
                 load_sem, send_sem, x_recv, share_recv, recv_c, recv_1, recv_2, recv_z):
    nz = sizes[0]
    rows, cols = x_hbm.shape
    half = rows // 2
    members, width, units = gate_hbm.shape
    experts = own_share.shape[0]
    here = place(sizes)
    z, x, y, c = here
    me = device(here)[0]
    axis = ((0, 1, 0, 0), (0, 0, 1, 0))
    other = (0, 0, 0, 1)
    ep_rels = [(d, e, 0, 0) for d in range(nz) for e in range(2) if d or e]
    greeted = ep_rels + [axis[1], other]

    sem = pltpu.get_barrier_semaphore()
    for rel in greeted:
        pl.semaphore_signal(sem, inc=1, device_id=device(moved(here, sizes, rel)), device_id_type=MESH)

    def number(rel):
        return ((rel[0] * 2 + rel[1]) * 2 + rel[2]) * 2 + rel[3]

    def slot(h, rel):
        group, member = device(moved(here, sizes, rel))
        return x_ref.at[pl.ds(pl.multiple_of(group * rows + h * half, half), half),
                        pl.ds(pl.multiple_of(member * cols, cols), cols)]

    own = pltpu.make_async_copy(
        x_hbm, x_ref.at[pl.ds(pl.multiple_of(me * rows, rows), rows),
                        pl.ds(pl.multiple_of(device(here)[1] * cols, cols), cols)], load_sem.at[0])
    ids = pltpu.make_async_copy(ids_hbm, ids_ref, load_sem.at[1])
    prob = pltpu.make_async_copy(prob_hbm, prob_ref, load_sem.at[2])
    for load in (own, ids, prob):
        load.start()
    loads = []
    for m in range(members):
        loads.append(pltpu.make_async_copy(gate_hbm.at[m], w_ref.at[m, :, pl.ds(0, units)], load_sem.at[3 + 3 * m]))
        loads.append(pltpu.make_async_copy(up_hbm.at[m], w_ref.at[m, :, pl.ds(units, units)], load_sem.at[4 + 3 * m]))
    for m in range(members):
        loads.append(pltpu.make_async_copy(down_hbm.at[m], down_ref.at[pl.ds(m * units, units), :], load_sem.at[5 + 3 * m]))
    for load in loads:
        load.start()

    ids.wait()
    prob.wait()
    expert = lax.broadcasted_iota(jnp.int32, (experts, rows), 0)
    share = jnp.zeros((experts, rows), jnp.float32)
    for k in range(ids_ref.shape[0]):
        share = share + jnp.where(expert == ids_ref[k:k + 1, :], prob_ref[k:k + 1, :], 0.0)
    own_share[...] = share
    own.wait()
    pl.semaphore_wait(sem, len(greeted))

    sends = []

    def push(src, dst, recv, step):
        copy = pltpu.make_async_remote_copy(
            src_ref=src, dst_ref=dst, send_sem=send_sem.at[len(sends)], recv_sem=recv,
            device_id=device(moved(here, sizes, step)), device_id_type=MESH)
        copy.start()
        sends.append(copy)

    def arrive(ref, recv):
        pltpu.make_async_copy(ref, ref, recv).wait()

    def send(h, rel, step):
        lands = tuple(r ^ s for r, s in zip(rel, step))
        push(slot(h, rel), slot(h, rel), x_recv.at[h, number(lands)], step)

    def landed(h, rel):
        arrive(slot(h, rel), x_recv.at[h, number(rel)])

    first = {0: axis[0], 1: axis[1]}
    second = {0: axis[1], 1: axis[0]}

    def pass_on(d, h):
        if d:
            landed(h, (d, 0, 0, 0))
        send(h, (d, 0, 0, 0), first[h])
        send(h, (d, 0, 0, 0), second[h])
        send(h, (d, 0, 0, 0), other)

    def pass_second(d):
        for h in range(2):
            rel = (d,) + first[h][1:]
            landed(h, rel)
            send(h, rel, second[h])
            send(h, rel, other)

    def pass_last(d):
        for h in range(2):
            for rel in ((d,) + second[h][1:], (d, 1, 1, 0)):
                landed(h, rel)
                send(h, rel, other)

    def whole(d):
        for h in range(2):
            for e in range(2):
                for f in range(2):
                    landed(h, (d, e, f, 1))

    eye = lax.broadcasted_iota(jnp.int32, (rows, rows), 0) == lax.broadcasted_iota(jnp.int32, (rows, rows), 1)

    def hidden(d, e):
        group = flip(z, d) * 2 + flip(x, e)
        block = x_ref[pl.ds(pl.multiple_of(group * rows, rows), rows), :]

        @pl.loop(0, members)
        def _(m):
            line = share_ref[group, pl.ds(me * members + m, 1), :]
            scale = jnp.sum(jnp.where(eye, jnp.broadcast_to(line, (rows, rows)), 0.0), axis=1, keepdims=True)
            both = jnp.dot(block, w_ref[m], preferred_element_type=jnp.float32)
            gate, up = both[:, :units], both[:, units:]
            hid_ref[d, e * rows:(e + 1) * rows, pl.ds(pl.multiple_of(m * units, 128), units)] = (
                jax.nn.silu(gate) * up * scale).astype(hid_ref.dtype)

    def down(d, g):
        @pl.loop(0, 2)
        def _(f):
            member = (y + f - 2 * y * f) * 2 + flip(c, g)
            at = pl.ds(pl.multiple_of(member * cols, cols), cols)
            part_ref[d, f, g] = jnp.dot(
                hid_ref[d], down_ref[:, at], preferred_element_type=jnp.float32).astype(part_ref.dtype)

    def rel_of(h, a, b):
        return (b, a) if h == 0 else (a, b)

    def local(h, a, b, d, g):
        e, f = rel_of(h, a, b)
        return part_ref.at[d, f, g, pl.ds(e * rows + h * half, half), :]

    out_first = {0: axis[1], 1: axis[0]}
    out_second = {0: axis[0], 1: axis[1]}

    def swap(d):
        for a, b in ((1, 1), (1, 0), (0, 1), (0, 0)):
            for h in range(2):
                push(local(h, a, b, d, 1), buf_c.at[h, a, b, d], recv_c.at[h, a, b, d], other)

    def add(dst, *srcs):
        chunk = 16

        @pl.loop(0, half // chunk)
        def _(i):
            at = pl.ds(pl.multiple_of(i * chunk, chunk), chunk)
            total = srcs[0][at, :].astype(jnp.float32)
            for src in srcs[1:]:
                total = total + src[at, :].astype(jnp.float32)
            dst[at, :] = total.astype(dst.dtype)

    def step_first(d):
        for b in (1, 0):
            for h in range(2):
                piece = buf_c.at[h, 1, b, d]
                arrive(piece, recv_c.at[h, 1, b, d])
                add(piece, piece, local(h, 1, b, d, 0))
                push(piece, buf_1.at[h, b, d], recv_1.at[h, b, d], out_first[h])

    def step_second(d):
        for h in range(2):
            piece = buf_c.at[h, 0, 1, d]
            arrive(piece, recv_c.at[h, 0, 1, d])
            arrive(buf_1.at[h, 1, d], recv_1.at[h, 1, d])
            add(piece, piece, local(h, 0, 1, d, 0), buf_1.at[h, 1, d])
            push(piece, buf_2.at[h, d], recv_2.at[h, d], out_second[h])

    def step_last(d):
        for h in range(2):
            piece = buf_c.at[h, 0, 0, d]
            arrive(piece, recv_c.at[h, 0, 0, d])
            arrive(buf_1.at[h, 0, d], recv_1.at[h, 0, d])
            arrive(buf_2.at[h, d], recv_2.at[h, d])
            srcs = (piece, local(h, 0, 0, d, 0), buf_1.at[h, 0, d], buf_2.at[h, d])
            if d:
                add(piece, *srcs)
                push(piece, buf_z.at[h, d - 1], recv_z.at[h, d - 1], (d, 0, 0, 0))
            else:
                for k in range(nz - 1):
                    arrive(buf_z.at[h, k], recv_z.at[h, k])
                add(out_ref.at[pl.ds(h * half, half), :], *srcs, *[buf_z.at[h, k] for k in range(nz - 1)])

    def send_far(d):
        for h in range(2):
            send(h, (0, 0, 0, 0), (d, 0, 0, 0))

    send_far(1)
    for h in range(2):
        pass_on(0, h)
    for i, rel in enumerate(ep_rels):
        push(own_share, share_ref.at[me], share_recv.at[i], rel)
    keep = pltpu.make_async_copy(own_share, share_ref.at[me], load_sem.at[3 + 3 * members])
    keep.start()
    for d in range(2, nz):
        send_far(d)
    pass_second(0)
    for h in range(2):
        pass_on(1, h)
    pass_last(0)
    for load in loads:
        load.wait()
    keep.wait()
    for i in range(len(ep_rels)):
        arrive(share_ref.at[0], share_recv.at[i])

    last = nz - 1
    for d in range(nz):
        whole(d)
        hidden(d, 0)
        if d < last:
            pass_second(d + 1)
        elif last > 2:
            step_second(last - 1)
        hidden(d, 1)
        if d + 2 < nz:
            for h in range(2):
                pass_on(d + 2, h)
        if d >= 2:
            down(d, 1)
            swap(d)
            down(d, 0)
            step_first(d)
        if d < last:
            pass_last(d + 1)
    step_last(last - 1)
    down(1, 1)
    swap(1)
    down(1, 0)
    step_second(last)
    step_first(1)
    down(0, 1)
    swap(0)
    down(0, 0)
    step_last(last)
    step_second(1)
    step_first(0)
    step_last(1)
    step_second(0)
    step_last(0)
    for copy in sends:
        copy.wait_send()


def layer_scratch(sizes, x, ids, prob, gate, down):
    nz = sizes[0]
    groups, parts = nz * sizes[1], sizes[2] * sizes[3]
    rows, cols = x.shape
    half = rows // 2
    members, width, units = gate.shape
    experts = groups * members
    n_send = 2 * (nz - 1 + 7 * nz) + groups - 1 + 2 * (4 * nz + 2 * nz + nz + nz - 1)
    buffers = [
        pltpu.VMEM((groups * rows, parts * cols), x.dtype),
        pltpu.VMEM(ids.shape, ids.dtype),
        pltpu.VMEM(prob.shape, prob.dtype),
        pltpu.VMEM((experts, rows), prob.dtype),
        pltpu.VMEM((groups, experts, rows), prob.dtype),
        pltpu.VMEM((members, width, 2 * units), gate.dtype),
        pltpu.VMEM((members * units, parts * cols), down.dtype),
        pltpu.VMEM((nz, 2 * rows, members * units), x.dtype),
        pltpu.VMEM((nz, 2, 2, 2 * rows, cols), x.dtype),
        pltpu.VMEM((2, 2, 2, nz, half, cols), x.dtype),
        pltpu.VMEM((2, 2, nz, half, cols), x.dtype),
        pltpu.VMEM((2, nz, half, cols), x.dtype),
        pltpu.VMEM((2, nz - 1, half, cols), x.dtype),
    ]
    semaphores = [
        pltpu.SemaphoreType.DMA((4 + 3 * members,)),
        pltpu.SemaphoreType.DMA((n_send,)),
        pltpu.SemaphoreType.DMA((2, groups * parts)),
        pltpu.SemaphoreType.DMA((groups - 1,)),
        pltpu.SemaphoreType.DMA((2, 2, 2, nz)),
        pltpu.SemaphoreType.DMA((2, 2, nz)),
        pltpu.SemaphoreType.DMA((2, nz)),
        pltpu.SemaphoreType.DMA((2, nz - 1)),
    ]
    return buffers, semaphores


def layer(sizes, x, ids, prob, gate, up, down):
    buffers, semaphores = layer_scratch(sizes, x, ids, prob, gate, down)
    return pl.pallas_call(
        functools.partial(layer_kernel, sizes),
        out_shape=jax.ShapeDtypeStruct(x.shape, x.dtype),
        in_specs=[pl.BlockSpec(memory_space=pl.ANY)] * 6,
        out_specs=pl.BlockSpec(memory_space=pltpu.VMEM),
        scratch_shapes=buffers + semaphores,
        compiler_params=pltpu.CompilerParams(collective_id=0, has_side_effects=True, vmem_limit_bytes=60 << 20),
        name="layer",
    )(x, ids, prob, gate, up, down)


def hidden_kernel(x_ref, w_ref, gate_ref, up_ref, out_ref):
    gate = jnp.dot(x_ref[...], gate_ref[0], preferred_element_type=jnp.float32)
    up = jnp.dot(x_ref[...], up_ref[0], preferred_element_type=jnp.float32)
    out_ref[...] = (jax.nn.silu(gate) * up * w_ref[0]).astype(out_ref.dtype)


def down_kernel(h_ref, down_ref, out_ref):
    out_ref[...] = jnp.dot(h_ref[...], down_ref[...], preferred_element_type=jnp.float32).astype(out_ref.dtype)


def tile_of(total, wanted):
    while total % wanted:
        wanted //= 2
    return wanted


def hidden_units(x, scale, gate_weight, up_weight):
    members, width, units = gate_weight.shape
    rows = x.shape[0]
    tile = tile_of(rows, 256)
    return pl.pallas_call(
        hidden_kernel,
        grid=(members, rows // tile),
        out_shape=jax.ShapeDtypeStruct((rows, members * units), x.dtype),
        in_specs=[
            pl.BlockSpec((tile, width), lambda e, m: (m, 0)),
            pl.BlockSpec((1, tile, 1), lambda e, m: (e, m, 0)),
            pl.BlockSpec((1, width, units), lambda e, m: (e, 0, 0)),
            pl.BlockSpec((1, width, units), lambda e, m: (e, 0, 0)),
        ],
        out_specs=pl.BlockSpec((tile, units), lambda e, m: (m, e)),
        compiler_params=pltpu.CompilerParams(vmem_limit_bytes=40 << 20),
        name="hidden",
    )(x, scale, gate_weight, up_weight)


def down_product(hidden, down_weight):
    members, units, width = down_weight.shape
    rows = hidden.shape[0]
    down = down_weight.reshape(members * units, width)
    tile_n = tile_of(width, 512)
    tile_m = tile_of(rows, 1024)
    return pl.pallas_call(
        down_kernel,
        grid=(rows // tile_m, width // tile_n),
        out_shape=jax.ShapeDtypeStruct((rows, width), hidden.dtype),
        in_specs=[
            pl.BlockSpec((tile_m, members * units), lambda m, n: (m, 0)),
            pl.BlockSpec((members * units, tile_n), lambda m, n: (0, n)),
        ],
        out_specs=pl.BlockSpec((tile_m, tile_n), lambda m, n: (m, n)),
        compiler_params=pltpu.CompilerParams(vmem_limit_bytes=50 << 20),
        name="down",
    )(hidden, down)


def body(tokens, expert_ids, gate_prob, gate_weight, up_weight, down_weight):
    groups, parts = lax.axis_size("ep"), lax.axis_size("etp")
    members = gate_weight.shape[0]
    sizes = (groups // 2, 2, parts // 2, 2)
    rows = tokens.shape[0]
    square = groups > 4 and groups & (groups - 1) == 0 and parts == 4 and members * groups <= rows == 128
    if square:
        ids, prob = jnp.transpose(expert_ids), jnp.transpose(gate_prob)
        buffers = layer_scratch(sizes, tokens, ids, prob, gate_weight, down_weight)[0]
        size = sum(math.prod(b.shape) * b.dtype.itemsize for b in buffers)
        if size <= VMEM_BUDGET:
            return layer(sizes, tokens, ids, prob, gate_weight, up_weight, down_weight)
    numbers = jnp.arange(members * groups, dtype=jnp.int32)
    share = jnp.sum(jnp.where(expert_ids[:, :, None] == numbers, gate_prob[:, :, None], 0.0), axis=1)
    gathered = lax.all_gather(lax.all_gather(tokens, "ep", axis=0, tiled=True), "etp", axis=1, tiled=True)
    shares = lax.all_gather(share, "ep", axis=0, tiled=True)
    mine = lax.dynamic_slice_in_dim(shares, lax.axis_index("ep") * members, members, axis=1)
    hidden = hidden_units(gathered, jnp.transpose(mine)[:, :, None], gate_weight, up_weight)
    partial_sum = down_product(hidden, down_weight)
    summed = lax.psum_scatter(partial_sum, "etp", scatter_dimension=1, tiled=True)
    return lax.psum_scatter(summed, "ep", scatter_dimension=0, tiled=True)


def solution(mesh):
    in_specs = (
        P("ep", "etp"),
        P("ep", None),
        P("ep", None),
        P("ep", None, "etp"),
        P("ep", None, "etp"),
        P("ep", "etp", None),
    )
    out_specs = P("ep", "etp")
    return jax.shard_map(body, mesh=mesh, in_specs=in_specs, out_specs=out_specs, check_vma=False)
```

```python
import functools
import math

import jax
import jax.numpy as jnp
from jax import lax
from jax.experimental import pallas as pl
from jax.experimental.pallas import tpu as pltpu
from jax.sharding import PartitionSpec as P

MESH = pl.DeviceIdType.MESH
VMEM_BUDGET = 56 << 20


def place(sizes):
    ep, etp = lax.axis_index("ep"), lax.axis_index("etp")
    return (ep // 2, ep % 2, etp // 2, etp % 2)


def flip(at, bits):
    bit = 1
    while bit <= bits:
        if bits & bit:
            at = at + bit - 2 * bit * ((at // bit) % 2)
        bit *= 2
    return at


def moved(here, sizes, rel):
    return tuple(flip(h, r) for h, r in zip(here, rel))


def device(at):
    z, x, y, c = at
    return (z * 2 + x, y * 2 + c)


def layer_kernel(sizes, x_hbm, ids_hbm, prob_hbm, gate_hbm, up_hbm, down_hbm, out_ref,
                 x_ref, ids_ref, prob_ref, own_share, share_ref, w_ref, down_ref, hid_ref, part_ref,
                 buf_c, buf_1, buf_2, buf_z, late_c, late_zs, late_1, late_2, scale_ref,
                 load_sem, send_sem, x_recv, share_recv, recv_c, recv_1, recv_2, recv_z,
                 recv_lc, recv_lz, recv_l1, recv_l2):
    nz = sizes[0]
    rows, cols = x_hbm.shape
    members, width, units = gate_hbm.shape
    experts = own_share.shape[0]
    here = place(sizes)
    z, x, y, c = here
    me = device(here)[0]
    axis = ((0, 1, 0, 0), (0, 0, 1, 0))
    other = (0, 0, 0, 1)
    ep_rels = [(d, e, 0, 0) for d in range(nz) for e in range(2) if d or e]
    greeted = ep_rels + [axis[1], other]

    sem = pltpu.get_barrier_semaphore()
    for rel in greeted:
        pl.semaphore_signal(sem, inc=1, device_id=device(moved(here, sizes, rel)), device_id_type=MESH)

    inner = (z + z // 2) % 2
    is_inner, is_outer = inner == 1, inner == 0
    planes = tuple(flip(z, s) for s in range(nz))
    pair, across = planes[1], planes[3]
    cuts = cuts_of(rows)

    def number(s, e, f, g):
        return ((s * 2 + e) * 2 + f) * 2 + g

    def slot(k, s, e, f, g):
        group = planes[s] * 2 + flip(x, e)
        member = flip(y, f) * 2 + flip(c, g)
        start, size = cuts[k]
        return x_ref.at[pl.ds(pl.multiple_of(group * rows + start, 16), size),
                        pl.ds(pl.multiple_of(member * cols, cols), cols)]

    own = pltpu.make_async_copy(
        x_hbm, x_ref.at[pl.ds(pl.multiple_of(me * rows, rows), rows),
                        pl.ds(pl.multiple_of(device(here)[1] * cols, cols), cols)], load_sem.at[0])
    ids = pltpu.make_async_copy(ids_hbm, ids_ref, load_sem.at[1])
    prob = pltpu.make_async_copy(prob_hbm, prob_ref, load_sem.at[2])
    for load in (own, ids, prob):
        load.start()
    loads = []
    for m in range(members):
        loads.append(pltpu.make_async_copy(gate_hbm.at[m], w_ref.at[m, :, pl.ds(0, units)], load_sem.at[3 + 3 * m]))
        loads.append(pltpu.make_async_copy(up_hbm.at[m], w_ref.at[m, :, pl.ds(units, units)], load_sem.at[4 + 3 * m]))
    for m in range(members):
        loads.append(pltpu.make_async_copy(down_hbm.at[m], down_ref.at[pl.ds(m * units, units), :], load_sem.at[5 + 3 * m]))
    for load in loads:
        load.start()

    ids.wait()
    prob.wait()
    expert = lax.broadcasted_iota(jnp.int32, (experts, rows), 0)
    share = jnp.zeros((experts, rows), jnp.float32)
    for k in range(ids_ref.shape[0]):
        share = share + jnp.where(expert == ids_ref[k:k + 1, :], prob_ref[k:k + 1, :], 0.0)
    own_share[...] = share
    own.wait()
    pl.semaphore_wait(sem, len(greeted))

    sends, relays = [], []

    def push(src, dst, recv, at, kept=sends):
        copy = pltpu.make_async_remote_copy(
            src_ref=src, dst_ref=dst, send_sem=send_sem.at[len(sends) + len(relays)], recv_sem=recv,
            device_id=device(at), device_id_type=MESH)
        copy.start()
        kept.append(copy if kept is sends else (len(sends) + len(relays), src.shape))

    def arrive(ref, recv):
        pltpu.make_async_copy(ref, ref, recv).wait()

    def send(k, s, e, f, step):
        push(slot(k, s, e, f, 0), slot(k, s, e, f, 0),
             x_recv.at[k, number(s, e ^ step[1], f ^ step[2], step[3])], moved(here, sizes, step))

    def send_z(k, s, e, f, to, lands, kept=sends):
        push(slot(k, s, e, f, 0), slot(k, s, e, f, 0), x_recv.at[k, number(lands, e, f, 0)], (to, x, y, c), kept)

    def landed(k, s, e, f, g=0):
        arrive(slot(k, s, e, f, g), x_recv.at[k, number(s, e, f, g)])

    def route(s):
        return ((s % 2, axis[0], axis[1]), (1 - s % 2, axis[1], axis[0]))

    def start_z():
        for k in range(2):
            send_z(k, 0, 0, 0, pair, 1)

        @pl.when(is_inner)
        def _():
            for k in range(2):
                send_z(k, 0, 0, 0, across, 3, relays)

    def start_late():
        if len(cuts) > 2:
            send(2, 0, 0, 0, axis[0])
            send(2, 0, 0, 0, axis[1])
            send(2, 0, 0, 0, other)

    def late_second():
        if len(cuts) > 2:
            landed(2, 0, 1, 0)
            send(2, 0, 1, 0, axis[1])
            send(2, 0, 1, 0, other)

    def late_z():
        if len(cuts) > 2:
            for e, f in ((0, 1), (1, 1)):
                landed(2, 0, e, f)
                send(2, 0, e, f, other)
            for e in range(2):
                for f in range(2):
                    send_z(2, 0, e, f, pair, 1)

            @pl.when(is_inner)
            def _():
                for e in range(2):
                    for f in range(2):
                        send_z(2, 0, e, f, across, 3, relays)

    hops = {1: (across, 2), 2: (pair, 3), 3: (pair, 2)}

    def relay(s):
        @pl.when(is_inner)
        def _():
            for k in range(2):
                landed(k, s, 0, 0)
                send_z(k, s, 0, 0, *hops[s], relays)

    def meet(s):
        @pl.when(is_outer)
        def _():
            for k in range(2):
                landed(k, s, 0, 0)

    def late_relay(s):
        if len(cuts) > 2:
            @pl.when(is_inner)
            def _():
                for e in range(2):
                    for f in range(2):
                        landed(2, s, e, f)
                        send_z(2, s, e, f, *hops[s], relays)

    def late_meet(s):
        if len(cuts) > 2:
            @pl.when(is_outer)
            def _():
                for e in range(2):
                    for f in range(2):
                        landed(2, s, e, f)

            for e in range(2):
                for f in range(2):
                    send(2, s, e, f, other)

    def pass_on(s):
        for k, first, second in route(s):
            send(k, s, 0, 0, first)
        for k, first, second in route(s):
            send(k, s, 0, 0, second)
        for k in range(2):
            send(k, s, 0, 0, other)

    def pass_second(s):
        for k, first, second in route(s):
            e, f = first[1], first[2]
            landed(k, s, e, f)
            send(k, s, e, f, second)
            send(k, s, e, f, other)

    def pass_last(s):
        for k, first, second in route(s):
            for e, f in (second[1:3], (1, 1)):
                landed(k, s, e, f)
                send(k, s, e, f, other)

    def whole(s):
        for k in range(len(cuts)):
            for e in range(2):
                for f in range(2):
                    landed(k, s, e, f, 1)

    eye = lax.broadcasted_iota(jnp.int32, (rows, rows), 0) == lax.broadcasted_iota(jnp.int32, (rows, rows), 1)

    def spread(s):
        for e in range(2):
            for m in range(members):
                line = share_ref[planes[s] * 2 + flip(x, e), pl.ds(me * members + m, 1), :]
                scale = jnp.sum(jnp.where(eye, jnp.broadcast_to(line, (rows, rows)), 0.0), axis=1, keepdims=True)
                scale_ref[s, e, m] = jnp.broadcast_to(scale, (rows, rows))

    def hidden(s, e):
        group = planes[s] * 2 + flip(x, e)
        block = x_ref[pl.ds(pl.multiple_of(group * rows, rows), rows), :]
        for m in range(members):
            both = jnp.dot(block, w_ref[m], preferred_element_type=jnp.float32)
            gate, up = both[:, :units], both[:, units:]
            scale = jnp.concatenate([scale_ref[s, e, m]] * (units // rows), axis=1)
            hid_ref[s, e * rows:(e + 1) * rows, m * units:(m + 1) * units] = (
                jax.nn.silu(gate) * up * scale).astype(hid_ref.dtype)

    def down(s, g):
        @pl.loop(0, 2, unroll=True)
        def _(f):
            member = (y + f - 2 * y * f) * 2 + flip(c, g)
            at = pl.ds(pl.multiple_of(member * cols, cols), cols)
            part_ref[s, f, g] = jnp.dot(
                hid_ref[s], down_ref[:, at], preferred_element_type=jnp.float32).astype(part_ref.dtype)

    spans = spans_of(rows)
    tail = rows - spans[1][0] - spans[1][1]

    def x_first(h, s):
        return (h + s) % 2 == 1

    def local(h, a, b, s, g):
        e, f = (a, b) if x_first(h, s) else (b, a)
        return part_ref.at[s, f, g, pl.ds(e * rows + spans[h][0], spans[h][1]), :]

    def local_late(e, f, s, g):
        return part_ref.at[s, f, g, pl.ds((e + 1) * rows - tail, tail), :]

    def piece_c(h, a, b, s):
        return buf_c.at[h, a, b, s, pl.ds(0, spans[h][1]), :]

    def piece_1(h, b, s):
        return buf_1.at[h, b, s, pl.ds(0, spans[h][1]), :]

    def piece_2(h, s):
        return buf_2.at[h, s, pl.ds(0, spans[h][1]), :]

    def piece_z(h, k):
        return buf_z.at[h, k, pl.ds(0, spans[h][1]), :]

    def swap(s):
        there = moved(here, sizes, other)
        for a, b in ((1, 1), (1, 0), (0, 1), (0, 0)):
            for h in range(2):
                push(local(h, a, b, s, 1), piece_c(h, a, b, s), recv_c.at[h, a, b, s], there)
        for e in range(2):
            for f in range(2):
                push(local_late(e, f, s, 1), late_c.at[s, e, f], recv_lc.at[s, e, f], there)

    def add(dst, *srcs):
        chunk = 16

        @pl.loop(0, dst.shape[0] // chunk)
        def _(i):
            at = pl.ds(pl.multiple_of(i * chunk, chunk), chunk)
            total = srcs[0][at, :].astype(jnp.float32)
            for src in srcs[1:]:
                total = total + src[at, :].astype(jnp.float32)
            dst[at, :] = total.astype(dst.dtype)

    def step_first(s, b):
        for h in range(2):
            piece = piece_c(h, 1, b, s)
            arrive(piece, recv_c.at[h, 1, b, s])
            add(piece, piece, local(h, 1, b, s, 0))
            push(piece, piece_1(h, b, s), recv_1.at[h, b, s], moved(here, sizes, axis[1 - x_first(h, s)]))

    def step_second(s):
        for h in range(2):
            piece = piece_c(h, 0, 1, s)
            arrive(piece, recv_c.at[h, 0, 1, s])
            arrive(piece_1(h, 1, s), recv_1.at[h, 1, s])
            add(piece, piece, local(h, 0, 1, s, 0), piece_1(h, 1, s))
            push(piece, piece_2(h, s), recv_2.at[h, s], moved(here, sizes, axis[int(x_first(h, s))]))

    def step_last(s):
        for h in range(2):
            piece = piece_c(h, 0, 0, s)
            arrive(piece, recv_c.at[h, 0, 0, s])
            arrive(piece_1(h, 0, s), recv_1.at[h, 0, s])
            arrive(piece_2(h, s), recv_2.at[h, s])
            srcs = (piece, local(h, 0, 0, s, 0), piece_1(h, 0, s), piece_2(h, s))
            for k in {0: (0, 2), 3: (1,)}.get(s, ()):
                arrive(piece_z(h, k), recv_z.at[h, k])
                srcs += (piece_z(h, k),)
            if s:
                add(piece, *srcs)
                push(piece, piece_z(h, s - 1), recv_z.at[h, s - 1], (across if s == 3 else pair, x, y, c))
            else:
                add(out_ref.at[pl.ds(*spans[h]), :], *srcs)

    def late_out(s):
        for e in range(2):
            for f in range(2):
                piece = late_c.at[s, e, f]
                arrive(piece, recv_lc.at[s, e, f])
                srcs = (piece, local_late(e, f, s, 0))
                for k in {0: (0, 2), 3: (1,)}.get(s, ()):
                    arrive(late_zs.at[k, e, f], recv_lz.at[k, e, f])
                    srcs += (late_zs.at[k, e, f],)
                add(piece, *srcs)
                if s:
                    push(piece, late_zs.at[s - 1, e, f], recv_lz.at[s - 1, e, f],
                         (across if s == 3 else pair, x, y, c))

    ways = [(i, pl.ds(i * 16, 16)) for i in range(tail // 16)]

    def late_piece(i, a, b, at):
        e, f = (b, a) if i else (a, b)
        return late_c.at[0, e, f, at, :]

    def late_first():
        for b in (1, 0):
            for i, at in ways:
                push(late_piece(i, 1, b, at), late_1.at[i, b], recv_l1.at[i, b], moved(here, sizes, axis[i]))

    def late_next():
        for i, at in ways:
            piece = late_piece(i, 0, 1, at)
            arrive(late_1.at[i, 1], recv_l1.at[i, 1])
            add(piece, piece, late_1.at[i, 1])
            push(piece, late_2.at[i], recv_l2.at[i], moved(here, sizes, axis[1 - i]))

    def late_last():
        for i, at in ways:
            arrive(late_1.at[i, 0], recv_l1.at[i, 0])
            arrive(late_2.at[i], recv_l2.at[i])
            add(out_ref.at[pl.ds(rows - tail + i * 16, 16), :], late_piece(i, 0, 0, at), late_1.at[i, 0], late_2.at[i])

    keep = pltpu.make_async_copy(own_share, share_ref.at[me], load_sem.at[3 + 3 * members])

    def send_shares():
        for i, rel in enumerate(ep_rels):
            push(own_share, share_ref.at[me], share_recv.at[i], moved(here, sizes, rel))
        keep.start()

    def wait_loads():
        for load in loads:
            load.wait()
        keep.wait()
        for i in range(len(ep_rels)):
            arrive(share_ref.at[0], share_recv.at[i])
        for s in range(nz):
            spread(s)

    start_z()
    start_late()
    pass_on(0)
    send_shares()
    late_second()
    pass_second(0)
    relay(1)
    meet(1)
    pass_on(1)
    relay(3)
    late_z()
    wait_loads()
    pass_last(0)
    relay(2)
    meet(2)
    pass_on(2)
    pass_second(1)
    whole(0)
    hidden(0, 0)
    late_relay(1)
    late_relay(3)
    meet(3)
    pass_on(3)
    hidden(0, 1)
    pass_second(2)
    late_meet(1)
    pass_last(1)
    whole(1)
    hidden(1, 0)
    late_relay(2)
    hidden(1, 1)
    pass_second(3)
    down(1, 1)
    swap(1)
    down(1, 0)
    late_meet(2)
    pass_last(2)
    step_first(1, 1)
    late_out(1)
    whole(2)
    hidden(2, 0)
    hidden(2, 1)
    late_meet(3)
    pass_last(3)
    step_first(1, 0)
    down(2, 1)
    swap(2)
    down(2, 0)
    whole(3)
    step_first(2, 1)
    step_first(2, 0)
    hidden(3, 0)
    late_out(2)
    hidden(3, 1)
    down(3, 1)
    swap(3)
    step_second(2)
    down(3, 0)
    step_first(3, 1)
    step_first(3, 0)
    step_last(2)
    late_out(3)
    down(0, 1)
    swap(0)
    down(0, 0)
    step_second(3)
    step_second(1)
    step_first(0, 1)
    step_first(0, 0)
    step_last(3)
    step_last(1)
    step_second(0)
    late_out(0)
    late_first()
    late_next()
    step_last(0)
    late_last()
    for copy in sends:
        copy.wait_send()

    @pl.when(is_inner)
    def _():
        for at, (size, span) in relays:
            done = x_ref.at[pl.ds(0, size), pl.ds(0, span)]
            pltpu.make_async_copy(done, done, send_sem.at[at]).wait()


def cuts_of(rows):
    late = 16
    most = 64
    return [(0, most), (most, rows - late - most)] + ([(rows - late, late)] if late else [])


def spans_of(rows):
    late = 16
    most = (rows - late + 16) // 32 * 16
    return [(0, most), (most, rows - late - most)]


def layer_scratch(sizes, x, ids, prob, gate, down):
    nz = sizes[0]
    groups, parts = nz * sizes[1], sizes[2] * sizes[3]
    rows, cols = x.shape
    spans = spans_of(rows)
    half, tail = spans[0][1], rows - spans[1][0] - spans[1][1]
    members, width, units = gate.shape
    experts = groups * members
    n_send = 32 * nz + 24 * nz + groups - 1 + 2 * (4 * nz + 2 * nz + nz + nz - 1) + 8 * nz + 8
    buffers = [
        pltpu.VMEM((groups * rows, parts * cols), x.dtype),
        pltpu.VMEM(ids.shape, ids.dtype),
        pltpu.VMEM(prob.shape, prob.dtype),
        pltpu.VMEM((experts, rows), prob.dtype),
        pltpu.VMEM((groups, experts, rows), prob.dtype),
        pltpu.VMEM((members, width, 2 * units), gate.dtype),
        pltpu.VMEM((members * units, parts * cols), down.dtype),
        pltpu.VMEM((nz, 2 * rows, members * units), x.dtype),
        pltpu.VMEM((nz, 2, 2, 2 * rows, cols), x.dtype),
        pltpu.VMEM((2, 2, 2, nz, half, cols), x.dtype),
        pltpu.VMEM((2, 2, nz, half, cols), x.dtype),
        pltpu.VMEM((2, nz, half, cols), x.dtype),
        pltpu.VMEM((2, nz - 1, half, cols), x.dtype),
        pltpu.VMEM((nz, 2, 2, tail, cols), x.dtype),
        pltpu.VMEM((nz - 1, 2, 2, tail, cols), x.dtype),
        pltpu.VMEM((tail // 16, 2, 16, cols), x.dtype),
        pltpu.VMEM((tail // 16, 16, cols), x.dtype),
        pltpu.VMEM((nz, 2, members, rows, rows), jnp.float32),
    ]
    semaphores = [
        pltpu.SemaphoreType.DMA((4 + 3 * members,)),
        pltpu.SemaphoreType.DMA((n_send,)),
        pltpu.SemaphoreType.DMA((3, groups * parts)),
        pltpu.SemaphoreType.DMA((groups - 1,)),
        pltpu.SemaphoreType.DMA((2, 2, 2, nz)),
        pltpu.SemaphoreType.DMA((2, 2, nz)),
        pltpu.SemaphoreType.DMA((2, nz)),
        pltpu.SemaphoreType.DMA((2, nz - 1)),
        pltpu.SemaphoreType.DMA((nz, 2, 2)),
        pltpu.SemaphoreType.DMA((nz - 1, 2, 2)),
        pltpu.SemaphoreType.DMA((tail // 16, 2)),
        pltpu.SemaphoreType.DMA((tail // 16,)),
    ]
    return buffers, semaphores


def layer(sizes, x, ids, prob, gate, up, down):
    buffers, semaphores = layer_scratch(sizes, x, ids, prob, gate, down)
    return pl.pallas_call(
        functools.partial(layer_kernel, sizes),
        out_shape=jax.ShapeDtypeStruct(x.shape, x.dtype),
        in_specs=[pl.BlockSpec(memory_space=pl.ANY)] * 6,
        out_specs=pl.BlockSpec(memory_space=pltpu.VMEM),
        scratch_shapes=buffers + semaphores,
        compiler_params=pltpu.CompilerParams(collective_id=0, has_side_effects=True, vmem_limit_bytes=60 << 20),
        name="layer",
    )(x, ids, prob, gate, up, down)


def hidden_kernel(x_ref, w_ref, gate_ref, up_ref, out_ref):
    gate = jnp.dot(x_ref[...], gate_ref[0], preferred_element_type=jnp.float32)
    up = jnp.dot(x_ref[...], up_ref[0], preferred_element_type=jnp.float32)
    out_ref[...] = (jax.nn.silu(gate) * up * w_ref[0]).astype(out_ref.dtype)


def down_kernel(h_ref, down_ref, out_ref):
    out_ref[...] = jnp.dot(h_ref[...], down_ref[...], preferred_element_type=jnp.float32).astype(out_ref.dtype)


def tile_of(total, wanted):
    while total % wanted:
        wanted //= 2
    return wanted


def hidden_units(x, scale, gate_weight, up_weight):
    members, width, units = gate_weight.shape
    rows = x.shape[0]
    tile = tile_of(rows, 256)
    return pl.pallas_call(
        hidden_kernel,
        grid=(members, rows // tile),
        out_shape=jax.ShapeDtypeStruct((rows, members * units), x.dtype),
        in_specs=[
            pl.BlockSpec((tile, width), lambda e, m: (m, 0)),
            pl.BlockSpec((1, tile, 1), lambda e, m: (e, m, 0)),
            pl.BlockSpec((1, width, units), lambda e, m: (e, 0, 0)),
            pl.BlockSpec((1, width, units), lambda e, m: (e, 0, 0)),
        ],
        out_specs=pl.BlockSpec((tile, units), lambda e, m: (m, e)),
        compiler_params=pltpu.CompilerParams(vmem_limit_bytes=40 << 20),
        name="hidden",
    )(x, scale, gate_weight, up_weight)


def down_product(hidden, down_weight):
    members, units, width = down_weight.shape
    rows = hidden.shape[0]
    down = down_weight.reshape(members * units, width)
    tile_n = tile_of(width, 512)
    tile_m = tile_of(rows, 1024)
    return pl.pallas_call(
        down_kernel,
        grid=(rows // tile_m, width // tile_n),
        out_shape=jax.ShapeDtypeStruct((rows, width), hidden.dtype),
        in_specs=[
            pl.BlockSpec((tile_m, members * units), lambda m, n: (m, 0)),
            pl.BlockSpec((members * units, tile_n), lambda m, n: (0, n)),
        ],
        out_specs=pl.BlockSpec((tile_m, tile_n), lambda m, n: (m, n)),
        compiler_params=pltpu.CompilerParams(vmem_limit_bytes=50 << 20),
        name="down",
    )(hidden, down)


def body(tokens, expert_ids, gate_prob, gate_weight, up_weight, down_weight):
    groups, parts = lax.axis_size("ep"), lax.axis_size("etp")
    members = gate_weight.shape[0]
    sizes = (groups // 2, 2, parts // 2, 2)
    rows = tokens.shape[0]
    square = groups == 8 and parts == 4 and members * groups <= rows == 128
    if square:
        ids, prob = jnp.transpose(expert_ids), jnp.transpose(gate_prob)
        buffers = layer_scratch(sizes, tokens, ids, prob, gate_weight, down_weight)[0]
        size = sum(math.prod(b.shape) * b.dtype.itemsize for b in buffers)
        if size <= VMEM_BUDGET:
            return layer(sizes, tokens, ids, prob, gate_weight, up_weight, down_weight)
    numbers = jnp.arange(members * groups, dtype=jnp.int32)
    share = jnp.sum(jnp.where(expert_ids[:, :, None] == numbers, gate_prob[:, :, None], 0.0), axis=1)
    gathered = lax.all_gather(lax.all_gather(tokens, "ep", axis=0, tiled=True), "etp", axis=1, tiled=True)
    shares = lax.all_gather(share, "ep", axis=0, tiled=True)
    mine = lax.dynamic_slice_in_dim(shares, lax.axis_index("ep") * members, members, axis=1)
    hidden = hidden_units(gathered, jnp.transpose(mine)[:, :, None], gate_weight, up_weight)
    partial_sum = down_product(hidden, down_weight)
    summed = lax.psum_scatter(partial_sum, "etp", scatter_dimension=1, tiled=True)
    return lax.psum_scatter(summed, "ep", scatter_dimension=0, tiled=True)


def solution(mesh):
    in_specs = (
        P("ep", "etp"),
        P("ep", None),
        P("ep", None),
        P("ep", None, "etp"),
        P("ep", None, "etp"),
        P("ep", "etp", None),
    )
    out_specs = P("ep", "etp")
    return jax.shard_map(body, mesh=mesh, in_specs=in_specs, out_specs=out_specs, check_vma=False)
```

```python
import functools
import math

import jax
import jax.numpy as jnp
from jax import lax
from jax.experimental import pallas as pl
from jax.experimental.pallas import tpu as pltpu
from jax.sharding import PartitionSpec as P

MESH = pl.DeviceIdType.MESH
VMEM_BUDGET = 56 << 20


def place(sizes):
    ep, etp = lax.axis_index("ep"), lax.axis_index("etp")
    return (ep // 2, ep % 2, etp // 2, etp % 2)


def flip(at, bits):
    bit = 1
    while bit <= bits:
        if bits & bit:
            at = at + bit - 2 * bit * ((at // bit) % 2)
        bit *= 2
    return at


def moved(here, sizes, rel):
    return tuple(flip(h, r) for h, r in zip(here, rel))


def device(at):
    z, x, y, c = at
    return (z * 2 + x, y * 2 + c)


def layer_kernel(sizes, x_hbm, ids_hbm, prob_hbm, gate_hbm, up_hbm, down_hbm, out_ref,
                 x_ref, ids_ref, prob_ref, own_share, share_ref, w_ref, down_ref, hid_ref, part_ref,
                 buf_c, buf_1, buf_2, buf_z, late_c, late_zs, late_1, late_2, scale_ref,
                 load_sem, send_sem, x_recv, z_recv, core_recv, late_recv, share_recv, recv_c, recv_1, recv_2, recv_z,
                 recv_lc, recv_lz, recv_l1, recv_l2):
    nz = sizes[0]
    rows, cols = x_hbm.shape
    members, width, units = gate_hbm.shape
    experts = own_share.shape[0]
    here = place(sizes)
    z, x, y, c = here
    me = device(here)[0]
    axis = ((0, 1, 0, 0), (0, 0, 1, 0))
    other = (0, 0, 0, 1)
    ep_rels = [(d, e, 0, 0) for d in range(nz) for e in range(2) if d or e]
    greeted = ep_rels + [axis[1], other]

    sem = pltpu.get_barrier_semaphore()
    for rel in greeted:
        pl.semaphore_signal(sem, inc=1, device_id=device(moved(here, sizes, rel)), device_id_type=MESH)

    inner = (z + z // 2) % 2
    is_inner, is_outer = inner == 1, inner == 0
    planes = tuple(flip(z, s) for s in range(nz))
    pair, across = planes[1], planes[3]
    cuts = cuts_of(rows)
    strips = strips_of(cuts)

    def number(s, e, f):
        return s * 3 + e * 2 + f - 1

    def slot(k, s, e, f, g):
        group = planes[s] * 2 + flip(x, e)
        member = flip(y, f) * 2 + flip(c, g)
        start, size = cuts[k]
        return x_ref.at[pl.ds(pl.multiple_of(group * rows + start, 16), size),
                        pl.ds(pl.multiple_of(member * cols, cols), cols)]

    own = pltpu.make_async_copy(
        x_hbm, x_ref.at[pl.ds(pl.multiple_of(me * rows, rows), rows),
                        pl.ds(pl.multiple_of(device(here)[1] * cols, cols), cols)], load_sem.at[0])
    ids = pltpu.make_async_copy(ids_hbm, ids_ref, load_sem.at[1])
    prob = pltpu.make_async_copy(prob_hbm, prob_ref, load_sem.at[2])
    for load in (own, ids, prob):
        load.start()
    loads = []
    for m in range(members):
        loads.append(pltpu.make_async_copy(gate_hbm.at[m], w_ref.at[m, :, pl.ds(0, units)], load_sem.at[3 + 3 * m]))
        loads.append(pltpu.make_async_copy(up_hbm.at[m], w_ref.at[m, :, pl.ds(units, units)], load_sem.at[4 + 3 * m]))
    for m in range(members):
        loads.append(pltpu.make_async_copy(down_hbm.at[m], down_ref.at[pl.ds(m * units, units), :], load_sem.at[5 + 3 * m]))
    for load in loads:
        load.start()

    ids.wait()
    prob.wait()
    expert = lax.broadcasted_iota(jnp.int32, (experts, rows), 0)
    share = jnp.zeros((experts, rows), jnp.float32)
    for k in range(ids_ref.shape[0]):
        share = share + jnp.where(expert == ids_ref[k:k + 1, :], prob_ref[k:k + 1, :], 0.0)
    own_share[...] = share
    own.wait()
    pl.semaphore_wait(sem, len(greeted))

    sends, relays, lines = [0], [], []

    def push(src, dst, recv, at, kept=sends):
        if kept is sends and sends[-1] + src.shape[0] > 1024:
            sends.append(0)
        kept.append(src.shape[0]) if kept is relays else kept.__setitem__(-1, kept[-1] + src.shape[0])
        pltpu.make_async_remote_copy(
            src_ref=src, dst_ref=dst, send_sem=send_sem.at[1 + len(sends) if kept is sends else 0], recv_sem=recv,
            device_id=device(at), device_id_type=MESH).start()

    def arrive_rows(count, recv):
        ref = x_ref.at[pl.ds(0, count), pl.ds(0, cols)]
        pltpu.make_async_copy(ref, ref, recv).wait()

    def arrive(ref, recv):
        pltpu.make_async_copy(ref, ref, recv).wait()

    def send(k, s, e, f, step):
        push(slot(k, s, e, f, 0), slot(k, s, e, f, 0),
             core_recv.at[s] if step[3] else x_recv.at[k, number(s, e ^ step[1], f ^ step[2])], moved(here, sizes, step))

    def send_z(k, s, e, f, to, lands, kept=sends):
        push(slot(k, s, e, f, 0), slot(k, s, e, f, 0), late_recv.at[lands], (to, x, y, c), kept)

    def strip(i, s):
        start, size = strips[i]
        return x_ref.at[pl.ds(pl.multiple_of((planes[s] * 2 + x) * rows + start, 16), size),
                        pl.ds(pl.multiple_of(device(here)[1] * cols, cols), cols)]

    def send_strip(i, s, to, lands, kept=sends):
        push(strip(i, s), strip(i, s), z_recv.at[i, lands], (to, x, y, c), kept)

    def strip_landed(i, s):
        arrive(strip(i, s), z_recv.at[i, s])

    def landed(k, s, e, f):
        arrive(slot(k, s, e, f, 0), x_recv.at[k, number(s, e, f)])

    def route(s):
        return ((s % 2, axis[0], axis[1]), (1 - s % 2, axis[1], axis[0]))

    def start_z():
        for i in range(len(strips)):
            send_strip(i, 0, pair, 1)

        @pl.when(is_inner)
        def _():
            for i in range(len(strips)):
                send_strip(i, 0, across, 3, relays)

    def start_late():
        if len(cuts) > 2:
            send(2, 0, 0, 0, axis[0])
            send(2, 0, 0, 0, axis[1])
            send(2, 0, 0, 0, other)

    def late_second():
        if len(cuts) > 2:
            landed(2, 0, 1, 0)
            send(2, 0, 1, 0, axis[1])
            send(2, 0, 1, 0, other)

    def late_z():
        if len(cuts) > 2:
            for e, f in ((0, 1), (1, 1)):
                landed(2, 0, e, f)
                send(2, 0, e, f, other)
            for e in range(2):
                for f in range(2):
                    send_z(2, 0, e, f, pair, 1)

            @pl.when(is_inner)
            def _():
                for e in range(2):
                    for f in range(2):
                        send_z(2, 0, e, f, across, 3, relays)

    hops = {1: (across, 2), 2: (pair, 3), 3: (pair, 2)}

    def relay(i, *which):
        @pl.when(is_inner)
        def _():
            for s in which:
                strip_landed(i, s)
                send_strip(i, s, *hops[s], relays)

    def meet(s):
        @pl.when(is_outer)
        def _():
            for i in range(len(strips)):
                strip_landed(i, s)

    def late_relay(s):
        if len(cuts) > 2:
            @pl.when(is_inner)
            def _():
                arrive_rows(4 * cuts[2][1], late_recv.at[s])
                for e in range(2):
                    for f in range(2):
                        send_z(2, s, e, f, *hops[s], relays)

    def late_meet(s):
        if len(cuts) > 2:
            @pl.when(is_outer)
            def _():
                arrive_rows(4 * cuts[2][1], late_recv.at[s])

            for e in range(2):
                for f in range(2):
                    send(2, s, e, f, other)

    def pass_on(s):
        for k, first, second in route(s):
            send(k, s, 0, 0, first)
        for k, first, second in route(s):
            send(k, s, 0, 0, second)
        for k in range(2):
            send(k, s, 0, 0, other)

    def pass_second(s, ks=(0, 1)):
        for k, first, second in route(s):
            if k not in ks:
                continue
            e, f = first[1], first[2]
            landed(k, s, e, f)
            send(k, s, e, f, second)
            send(k, s, e, f, other)

    def pass_last(s):
        for k, first, second in route(s):
            for e, f in (second[1:3], (1, 1)):
                landed(k, s, e, f)
                send(k, s, e, f, other)

    def whole(s):
        arrive_rows(4 * rows, core_recv.at[s])

    eye = lax.broadcasted_iota(jnp.int32, (rows, rows), 0) == lax.broadcasted_iota(jnp.int32, (rows, rows), 1)

    def spread(s):
        for e in range(2):
            for m in range(members):
                line = share_ref[planes[s] * 2 + flip(x, e), pl.ds(me * members + m, 1), :]
                scale = jnp.sum(jnp.where(eye, jnp.broadcast_to(line, (rows, rows)), 0.0), axis=1, keepdims=True)
                scale_ref[s, e, m] = jnp.broadcast_to(scale, (rows, rows))

    def hidden(s, e):
        group = planes[s] * 2 + flip(x, e)
        block = x_ref[pl.ds(pl.multiple_of(group * rows, rows), rows), :]
        for m in range(members):
            both = jnp.dot(block, w_ref[m], preferred_element_type=jnp.float32)
            gate, up = both[:, :units], both[:, units:]
            scale = jnp.concatenate([scale_ref[s, e, m]] * (units // rows), axis=1)
            hid_ref[s, e * rows:(e + 1) * rows, m * units:(m + 1) * units] = (
                jax.nn.silu(gate) * up * scale).astype(hid_ref.dtype)

    def down(s, g, es=(0, 1)):
        at_rows = pl.ds(es[0] * rows, len(es) * rows)

        @pl.loop(0, 2, unroll=True)
        def _(f):
            member = (y + f - 2 * y * f) * 2 + flip(c, g)
            at = pl.ds(pl.multiple_of(member * cols, cols), cols)
            part_ref[s, f, g, at_rows, :] = jnp.dot(
                hid_ref[s, at_rows, :], down_ref[:, at], preferred_element_type=jnp.float32).astype(part_ref.dtype)

    spans = spans_of(rows)
    tail = rows - spans[1][0] - spans[1][1]

    def x_first(h, s):
        return (h + s) % 2 == 1

    def local(h, a, b, s, g):
        e, f = (a, b) if x_first(h, s) else (b, a)
        return part_ref.at[s, f, g, pl.ds(e * rows + spans[h][0], spans[h][1]), :]

    def local_late(e, f, s, g):
        return part_ref.at[s, f, g, pl.ds((e + 1) * rows - tail, tail), :]

    def piece_c(h, a, b, s):
        return buf_c.at[h, a, b, s, pl.ds(0, spans[h][1]), :]

    def piece_1(h, b, s):
        return buf_1.at[h, b, s, pl.ds(0, spans[h][1]), :]

    def piece_2(h, s):
        return buf_2.at[h, s, pl.ds(0, spans[h][1]), :]

    def piece_z(h, k):
        return buf_z.at[h, k, pl.ds(0, spans[h][1]), :]

    def swap(s, es=(0, 1)):
        there = moved(here, sizes, other)
        for a, b in ((1, 1), (1, 0), (0, 1), (0, 0)):
            for h in range(2):
                if (a if x_first(h, s) else b) in es:
                    push(local(h, a, b, s, 1), piece_c(h, a, b, s), recv_c.at[a, b, s], there)
        for e in es:
            for f in range(2):
                push(local_late(e, f, s, 1), late_c.at[s, e, f], recv_lc.at[s], there)

    def add(dst, *srcs):
        chunk = 16

        @pl.loop(0, dst.shape[0] // chunk)
        def _(i):
            at = pl.ds(pl.multiple_of(i * chunk, chunk), chunk)
            total = srcs[0][at, :].astype(jnp.float32)
            for src in srcs[1:]:
                total = total + src[at, :].astype(jnp.float32)
            dst[at, :] = total.astype(dst.dtype)

    def step_first(s, b):
        arrive_rows(rows - tail, recv_c.at[1, b, s])
        for h in range(2):
            piece = piece_c(h, 1, b, s)
            add(piece, piece, local(h, 1, b, s, 0))
            push(piece, piece_1(h, b, s), recv_1.at[h, b, s], moved(here, sizes, axis[1 - x_first(h, s)]))

    def step_second(s):
        arrive_rows(rows - tail, recv_c.at[0, 1, s])
        for h in range(2):
            piece = piece_c(h, 0, 1, s)
            arrive(piece_1(h, 1, s), recv_1.at[h, 1, s])
            add(piece, piece, local(h, 0, 1, s, 0), piece_1(h, 1, s))
            push(piece, piece_2(h, s), recv_2.at[h, s], moved(here, sizes, axis[int(x_first(h, s))]))

    def step_last(s):
        arrive_rows(rows - tail, recv_c.at[0, 0, s])
        for h in range(2):
            piece = piece_c(h, 0, 0, s)
            arrive(piece_1(h, 0, s), recv_1.at[h, 0, s])
            arrive(piece_2(h, s), recv_2.at[h, s])
            srcs = (piece, local(h, 0, 0, s, 0), piece_1(h, 0, s), piece_2(h, s))
            for k in {0: (0, 2), 3: (1,)}.get(s, ()):
                arrive(piece_z(h, k), recv_z.at[h, k])
                srcs += (piece_z(h, k),)
            if s:
                add(piece, *srcs)
                push(piece, piece_z(h, s - 1), recv_z.at[h, s - 1], (across if s == 3 else pair, x, y, c))
            else:
                add(out_ref.at[pl.ds(*spans[h]), :], *srcs)

    def late_out(s):
        more = {0: (0, 2), 3: (1,)}.get(s, ())
        arrive_rows(4 * tail, recv_lc.at[s])
        for k in more:
            arrive_rows(4 * tail, recv_lz.at[k])
        for e in range(2):
            for f in range(2):
                piece = late_c.at[s, e, f]
                add(piece, piece, local_late(e, f, s, 0), *[late_zs.at[k, e, f] for k in more])
                if s:
                    push(piece, late_zs.at[s - 1, e, f], recv_lz.at[s - 1], (across if s == 3 else pair, x, y, c))

    ways = [(i, pl.ds(i * 16, 16)) for i in range(tail // 16)]

    def late_piece(i, a, b, at):
        e, f = (b, a) if i else (a, b)
        return late_c.at[0, e, f, at, :]

    def late_first():
        for b in (1, 0):
            for i, at in ways:
                push(late_piece(i, 1, b, at), late_1.at[i, b], recv_l1.at[i, b], moved(here, sizes, axis[i]))

    def late_next():
        for i, at in ways:
            piece = late_piece(i, 0, 1, at)
            arrive(late_1.at[i, 1], recv_l1.at[i, 1])
            add(piece, piece, late_1.at[i, 1])
            push(piece, late_2.at[i], recv_l2.at[i], moved(here, sizes, axis[1 - i]))

    def late_last():
        for i, at in ways:
            arrive(late_1.at[i, 0], recv_l1.at[i, 0])
            arrive(late_2.at[i], recv_l2.at[i])
            add(out_ref.at[pl.ds(rows - tail + i * 16, 16), :], late_piece(i, 0, 0, at), late_1.at[i, 0], late_2.at[i])

    keep = pltpu.make_async_copy(own_share, share_ref.at[me], load_sem.at[3 + 3 * members])

    def send_shares():
        for rel in ep_rels:
            pltpu.make_async_remote_copy(
                src_ref=own_share, dst_ref=share_ref.at[me], send_sem=send_sem.at[1], recv_sem=share_recv,
                device_id=device(moved(here, sizes, rel)), device_id_type=MESH).start()
        keep.start()

    def wait_loads():
        for load in loads:
            load.wait()
        keep.wait()
        others = share_ref.at[pl.ds(0, len(ep_rels))]
        pltpu.make_async_copy(others, others, share_recv).wait()
        for s in range(nz):
            spread(s)

    start_z()
    start_late()
    pass_on(0)
    send_shares()
    late_second()
    relay(0, 1, 3)
    relay(1, 1, 3)
    pass_second(0)
    relay(2, 1, 3)
    meet(1)
    pass_on(1)
    relay(0, 2)
    wait_loads()
    relay(1, 2)
    relay(2, 2)
    late_z()
    pass_last(0)
    meet(2)
    pass_on(2)
    pass_second(1)
    whole(0)
    hidden(0, 0)
    hidden(0, 1)
    pass_second(2)
    meet(3)
    pass_on(3)
    late_relay(1)
    late_relay(3)
    down(0, 1)
    swap(0)
    down(0, 0)
    late_meet(1)
    pass_last(1)
    whole(1)
    hidden(1, 0)
    late_relay(2)
    late_meet(2)
    pass_last(2)
    hidden(1, 1)
    pass_second(3)
    down(1, 1)
    swap(1)
    down(1, 0)
    step_first(1, 1)
    whole(2)
    hidden(2, 1)
    step_first(1, 0)
    hidden(2, 0)
    late_meet(3)
    pass_last(3)
    down(2, 1)
    swap(2)
    late_out(1)
    down(2, 0)
    step_first(2, 1)
    step_first(2, 0)
    whole(3)
    hidden(3, 1)
    late_out(2)
    down(3, 1, (1,))
    swap(3, (1,))
    down(3, 0, (1,))
    hidden(3, 0)
    step_second(2)
    step_first(3, 1)
    down(3, 1, (0,))
    swap(3, (0,))
    down(3, 0, (0,))
    step_first(3, 0)
    late_out(3)
    step_last(2)
    step_second(3)
    step_second(1)
    step_first(0, 1)
    step_first(0, 0)
    step_last(3)
    late_out(0)
    late_first()
    step_last(1)
    step_second(0)
    late_next()
    step_last(0)
    late_last()
    for i, count in enumerate(sends):
        arrive_rows(count, send_sem.at[2 + i])
    gone = share_ref.at[pl.ds(0, len(ep_rels))]
    pltpu.make_async_copy(gone, gone, send_sem.at[1]).wait()

    @pl.when(is_inner)
    def _():
        arrive_rows(sum(relays), send_sem.at[0])


def cuts_of(rows):
    late = 16
    most = 64
    return [(0, most), (most, rows - late - most)] + ([(rows - late, late)] if late else [])


def strips_of(cuts):
    (_, a), (start, b) = cuts[:2]
    return [(0, a // 32 * 16), (a // 32 * 16, a - a // 32 * 16), (start, b)]


def spans_of(rows):
    late = 16
    most = (rows - late + 16) // 32 * 16
    return [(0, most), (most, rows - late - most)]


def layer_scratch(sizes, x, ids, prob, gate, down):
    nz = sizes[0]
    groups, parts = nz * sizes[1], sizes[2] * sizes[3]
    rows, cols = x.shape
    spans = spans_of(rows)
    half, tail = spans[0][1], rows - spans[1][0] - spans[1][1]
    members, width, units = gate.shape
    experts = groups * members
    buffers = [
        pltpu.VMEM((groups * rows, parts * cols), x.dtype),
        pltpu.VMEM(ids.shape, ids.dtype),
        pltpu.VMEM(prob.shape, prob.dtype),
        pltpu.VMEM((experts, rows), prob.dtype),
        pltpu.VMEM((groups, experts, rows), prob.dtype),
        pltpu.VMEM((members, width, 2 * units), gate.dtype),
        pltpu.VMEM((members * units, parts * cols), down.dtype),
        pltpu.VMEM((nz, 2 * rows, members * units), x.dtype),
        pltpu.VMEM((nz, 2, 2, 2 * rows, cols), x.dtype),
        pltpu.VMEM((2, 2, 2, nz, half, cols), x.dtype),
        pltpu.VMEM((2, 2, nz, half, cols), x.dtype),
        pltpu.VMEM((2, nz, half, cols), x.dtype),
        pltpu.VMEM((2, nz - 1, half, cols), x.dtype),
        pltpu.VMEM((nz, 2, 2, tail, cols), x.dtype),
        pltpu.VMEM((nz - 1, 2, 2, tail, cols), x.dtype),
        pltpu.VMEM((tail // 16, 2, 16, cols), x.dtype),
        pltpu.VMEM((tail // 16, 16, cols), x.dtype),
        pltpu.VMEM((nz, 2, members, rows, rows), jnp.float32),
    ]
    semaphores = [pltpu.SemaphoreType.DMA(shape) for shape in (
        (4 + 3 * members,), (12,), (3, 3 * nz), (3, nz), (nz,), (nz,), (), (2, 2, nz), (2, 2, nz), (2, nz), (2, nz - 1),
        (nz,), (nz - 1,), (tail // 16, 2), (tail // 16,))]
    return buffers, semaphores


def layer(sizes, x, ids, prob, gate, up, down):
    buffers, semaphores = layer_scratch(sizes, x, ids, prob, gate, down)
    return pl.pallas_call(
        functools.partial(layer_kernel, sizes),
        out_shape=jax.ShapeDtypeStruct(x.shape, x.dtype),
        in_specs=[pl.BlockSpec(memory_space=pl.ANY)] * 6,
        out_specs=pl.BlockSpec(memory_space=pltpu.VMEM),
        scratch_shapes=buffers + semaphores,
        compiler_params=pltpu.CompilerParams(collective_id=0, has_side_effects=True, vmem_limit_bytes=60 << 20),
        name="layer",
    )(x, ids, prob, gate, up, down)


def hidden_kernel(x_ref, w_ref, gate_ref, up_ref, out_ref):
    gate = jnp.dot(x_ref[...], gate_ref[0], preferred_element_type=jnp.float32)
    up = jnp.dot(x_ref[...], up_ref[0], preferred_element_type=jnp.float32)
    out_ref[...] = (jax.nn.silu(gate) * up * w_ref[0]).astype(out_ref.dtype)


def down_kernel(h_ref, down_ref, out_ref):
    out_ref[...] = jnp.dot(h_ref[...], down_ref[...], preferred_element_type=jnp.float32).astype(out_ref.dtype)


def tile_of(total, wanted):
    while total % wanted:
        wanted //= 2
    return wanted


def hidden_units(x, scale, gate_weight, up_weight):
    members, width, units = gate_weight.shape
    rows = x.shape[0]
    tile = tile_of(rows, 256)
    return pl.pallas_call(
        hidden_kernel,
        grid=(members, rows // tile),
        out_shape=jax.ShapeDtypeStruct((rows, members * units), x.dtype),
        in_specs=[
            pl.BlockSpec((tile, width), lambda e, m: (m, 0)),
            pl.BlockSpec((1, tile, 1), lambda e, m: (e, m, 0)),
            pl.BlockSpec((1, width, units), lambda e, m: (e, 0, 0)),
            pl.BlockSpec((1, width, units), lambda e, m: (e, 0, 0)),
        ],
        out_specs=pl.BlockSpec((tile, units), lambda e, m: (m, e)),
        compiler_params=pltpu.CompilerParams(vmem_limit_bytes=40 << 20),
        name="hidden",
    )(x, scale, gate_weight, up_weight)


def down_product(hidden, down_weight):
    members, units, width = down_weight.shape
    rows = hidden.shape[0]
    down = down_weight.reshape(members * units, width)
    tile_n = tile_of(width, 512)
    tile_m = tile_of(rows, 1024)
    return pl.pallas_call(
        down_kernel,
        grid=(rows // tile_m, width // tile_n),
        out_shape=jax.ShapeDtypeStruct((rows, width), hidden.dtype),
        in_specs=[
            pl.BlockSpec((tile_m, members * units), lambda m, n: (m, 0)),
            pl.BlockSpec((members * units, tile_n), lambda m, n: (0, n)),
        ],
        out_specs=pl.BlockSpec((tile_m, tile_n), lambda m, n: (m, n)),
        compiler_params=pltpu.CompilerParams(vmem_limit_bytes=50 << 20),
        name="down",
    )(hidden, down)


def body(tokens, expert_ids, gate_prob, gate_weight, up_weight, down_weight):
    groups, parts = lax.axis_size("ep"), lax.axis_size("etp")
    members = gate_weight.shape[0]
    sizes = (groups // 2, 2, parts // 2, 2)
    rows = tokens.shape[0]
    square = groups == 8 and parts == 4 and members * groups <= rows == 128
    if square:
        ids, prob = jnp.transpose(expert_ids), jnp.transpose(gate_prob)
        buffers = layer_scratch(sizes, tokens, ids, prob, gate_weight, down_weight)[0]
        size = sum(math.prod(b.shape) * b.dtype.itemsize for b in buffers)
        if size <= VMEM_BUDGET:
            return layer(sizes, tokens, ids, prob, gate_weight, up_weight, down_weight)
    numbers = jnp.arange(members * groups, dtype=jnp.int32)
    share = jnp.sum(jnp.where(expert_ids[:, :, None] == numbers, gate_prob[:, :, None], 0.0), axis=1)
    gathered = lax.all_gather(lax.all_gather(tokens, "ep", axis=0, tiled=True), "etp", axis=1, tiled=True)
    shares = lax.all_gather(share, "ep", axis=0, tiled=True)
    mine = lax.dynamic_slice_in_dim(shares, lax.axis_index("ep") * members, members, axis=1)
    hidden = hidden_units(gathered, jnp.transpose(mine)[:, :, None], gate_weight, up_weight)
    partial_sum = down_product(hidden, down_weight)
    summed = lax.psum_scatter(partial_sum, "etp", scatter_dimension=1, tiled=True)
    return lax.psum_scatter(summed, "ep", scatter_dimension=0, tiled=True)


def solution(mesh):
    in_specs = (
        P("ep", "etp"),
        P("ep", None),
        P("ep", None),
        P("ep", None, "etp"),
        P("ep", None, "etp"),
        P("ep", "etp", None),
    )
    out_specs = P("ep", "etp")
    return jax.shard_map(body, mesh=mesh, in_specs=in_specs, out_specs=out_specs, check_vma=False)
```

```python
import functools
import math

import jax
import jax.numpy as jnp
from jax import lax
from jax.experimental import pallas as pl
from jax.experimental.pallas import tpu as pltpu
from jax.sharding import PartitionSpec as P

MESH = pl.DeviceIdType.MESH
VMEM_BUDGET = 56 << 20


def place(sizes):
    ep, etp = lax.axis_index("ep"), lax.axis_index("etp")
    return (ep // 2, ep % 2, etp // 2, etp % 2)


def flip(at, bits):
    bit = 1
    while bit <= bits:
        if bits & bit:
            at = at + bit - 2 * bit * ((at // bit) % 2)
        bit *= 2
    return at


def moved(here, sizes, rel):
    return tuple(flip(h, r) for h, r in zip(here, rel))


def device(at):
    z, x, y, c = at
    return (z * 2 + x, y * 2 + c)


def layer_kernel(sizes, x_hbm, ids_hbm, prob_hbm, gate_hbm, up_hbm, down_hbm, out_ref,
                 x_ref, ids_ref, prob_ref, own_share, share_ref, w_ref, down_ref, hid_ref, part_ref,
                 buf_c, buf_1, buf_2, buf_z, late_c, late_zs, late_1, late_2, scale_ref,
                 load_sem, send_sem, x_recv, z_recv, core_recv, late_recv, share_recv, recv_c, recv_1, recv_2, recv_z,
                 recv_lc, recv_lz, recv_l1, recv_l2):
    nz = sizes[0]
    rows, cols = x_hbm.shape
    members, width, units = gate_hbm.shape
    experts = own_share.shape[0]
    here = place(sizes)
    z, x, y, c = here
    me = device(here)[0]
    axis = ((0, 1, 0, 0), (0, 0, 1, 0))
    other = (0, 0, 0, 1)
    ep_rels = [(d, e, 0, 0) for d in range(nz) for e in range(2) if d or e]
    greeted = ep_rels + [axis[1], other]

    sem = pltpu.get_barrier_semaphore()
    for rel in greeted:
        pl.semaphore_signal(sem, inc=1, device_id=device(moved(here, sizes, rel)), device_id_type=MESH)

    inner = (z + z // 2) % 2
    is_inner, is_outer = inner == 1, inner == 0
    planes = tuple(flip(z, s) for s in range(nz))
    pair, across = planes[1], planes[3]
    cuts = cuts_of(rows)
    strips = strips_of(cuts)

    def number(s, e, f):
        return s * 3 + e * 2 + f - 1

    def slot(k, s, e, f, g):
        group = planes[s] * 2 + flip(x, e)
        member = flip(y, f) * 2 + flip(c, g)
        start, size = cuts[k]
        return x_ref.at[pl.ds(pl.multiple_of(group * rows + start, 16), size),
                        pl.ds(pl.multiple_of(member * cols, cols), cols)]

    own = pltpu.make_async_copy(
        x_hbm, x_ref.at[pl.ds(pl.multiple_of(me * rows, rows), rows),
                        pl.ds(pl.multiple_of(device(here)[1] * cols, cols), cols)], load_sem.at[0])
    ids = pltpu.make_async_copy(ids_hbm, ids_ref, load_sem.at[1])
    prob = pltpu.make_async_copy(prob_hbm, prob_ref, load_sem.at[2])
    for load in (own, ids, prob):
        load.start()
    loads = []
    for m in range(members):
        loads.append(pltpu.make_async_copy(gate_hbm.at[m], w_ref.at[m, :, pl.ds(0, units)], load_sem.at[3 + 3 * m]))
        loads.append(pltpu.make_async_copy(up_hbm.at[m], w_ref.at[m, :, pl.ds(units, units)], load_sem.at[4 + 3 * m]))
    for m in range(members):
        loads.append(pltpu.make_async_copy(down_hbm.at[m], down_ref.at[pl.ds(m * units, units), :], load_sem.at[5 + 3 * m]))
    for load in loads:
        load.start()

    ids.wait()
    prob.wait()
    expert = lax.broadcasted_iota(jnp.int32, (experts, rows), 0)
    share = jnp.zeros((experts, rows), jnp.float32)
    for k in range(ids_ref.shape[0]):
        share = share + jnp.where(expert == ids_ref[k:k + 1, :], prob_ref[k:k + 1, :], 0.0)
    own_share[...] = share
    own.wait()
    pl.semaphore_wait(sem, len(greeted))

    sends, relays, lines = [0], [], []

    def push(src, dst, recv, at, kept=sends):
        if kept is sends and sends[-1] + src.shape[0] > 1024:
            sends.append(0)
        kept.append(src.shape[0]) if kept is relays else kept.__setitem__(-1, kept[-1] + src.shape[0])
        pltpu.make_async_remote_copy(
            src_ref=src, dst_ref=dst, send_sem=send_sem.at[1 + len(sends) if kept is sends else 0], recv_sem=recv,
            device_id=device(at), device_id_type=MESH).start()

    def arrive_rows(count, recv):
        ref = x_ref.at[pl.ds(0, count), pl.ds(0, cols)]
        pltpu.make_async_copy(ref, ref, recv).wait()

    def arrive(ref, recv):
        pltpu.make_async_copy(ref, ref, recv).wait()

    def send(k, s, e, f, step):
        push(slot(k, s, e, f, 0), slot(k, s, e, f, 0),
             core_recv.at[s] if step[3] else x_recv.at[k, number(s, e ^ step[1], f ^ step[2])], moved(here, sizes, step))

    def send_z(k, s, e, f, to, lands, kept=sends):
        push(slot(k, s, e, f, 0), slot(k, s, e, f, 0), late_recv.at[lands], (to, x, y, c), kept)

    def strip(i, s):
        start, size = strips[i]
        return x_ref.at[pl.ds(pl.multiple_of((planes[s] * 2 + x) * rows + start, 16), size),
                        pl.ds(pl.multiple_of(device(here)[1] * cols, cols), cols)]

    def send_strip(i, s, to, lands, kept=sends):
        push(strip(i, s), strip(i, s), z_recv.at[i, lands], (to, x, y, c), kept)

    def strip_landed(i, s):
        arrive(strip(i, s), z_recv.at[i, s])

    def landed(k, s, e, f):
        arrive(slot(k, s, e, f, 0), x_recv.at[k, number(s, e, f)])

    def route(s):
        return ((s % 2, axis[0], axis[1]), (1 - s % 2, axis[1], axis[0]))

    def start_z():
        for i in range(len(strips)):
            send_strip(i, 0, pair, 1)

        @pl.when(is_inner)
        def _():
            for i in range(len(strips)):
                send_strip(i, 0, across, 3, relays)

    def start_late():
        if len(cuts) > 2:
            send(2, 0, 0, 0, axis[0])
            send(2, 0, 0, 0, axis[1])
            send(2, 0, 0, 0, other)

    def late_second():
        if len(cuts) > 2:
            landed(2, 0, 1, 0)
            send(2, 0, 1, 0, axis[1])
            send(2, 0, 1, 0, other)

    def late_z():
        if len(cuts) > 2:
            for e, f in ((0, 1), (1, 1)):
                landed(2, 0, e, f)
                send(2, 0, e, f, other)
            for e in range(2):
                for f in range(2):
                    send_z(2, 0, e, f, pair, 1)

            @pl.when(is_inner)
            def _():
                for e in range(2):
                    for f in range(2):
                        send_z(2, 0, e, f, across, 3, relays)

    hops = {1: (across, 2), 2: (pair, 3), 3: (pair, 2)}

    def relay(i, *which):
        @pl.when(is_inner)
        def _():
            for s in which:
                strip_landed(i, s)
                send_strip(i, s, *hops[s], relays)

    def meet(s):
        @pl.when(is_outer)
        def _():
            for i in range(len(strips)):
                strip_landed(i, s)

    def late_relay(s):
        if len(cuts) > 2:
            @pl.when(is_inner)
            def _():
                arrive_rows(4 * cuts[2][1], late_recv.at[s])
                for e in range(2):
                    for f in range(2):
                        send_z(2, s, e, f, *hops[s], relays)

    def late_meet(s):
        if len(cuts) > 2:
            @pl.when(is_outer)
            def _():
                arrive_rows(4 * cuts[2][1], late_recv.at[s])

            for e in range(2):
                for f in range(2):
                    send(2, s, e, f, other)

    def pass_on(s):
        for k, first, second in route(s):
            send(k, s, 0, 0, first)
        for k, first, second in route(s):
            send(k, s, 0, 0, second)
        for k in range(2):
            send(k, s, 0, 0, other)

    def pass_second(s, ks=(0, 1)):
        for k, first, second in route(s):
            if k not in ks:
                continue
            e, f = first[1], first[2]
            landed(k, s, e, f)
            send(k, s, e, f, second)
            send(k, s, e, f, other)

    def pass_last(s):
        for k, first, second in route(s):
            for e, f in (second[1:3], (1, 1)):
                landed(k, s, e, f)
                send(k, s, e, f, other)

    def whole(s):
        arrive_rows(4 * rows, core_recv.at[s])

    eye = lax.broadcasted_iota(jnp.int32, (rows, rows), 0) == lax.broadcasted_iota(jnp.int32, (rows, rows), 1)

    def spread(s):
        for e in range(2):
            for m in range(members):
                line = share_ref[planes[s] * 2 + flip(x, e), pl.ds(me * members + m, 1), :]
                scale = jnp.sum(jnp.where(eye, jnp.broadcast_to(line, (rows, rows)), 0.0), axis=1, keepdims=True)
                scale_ref[s, e, m] = jnp.broadcast_to(scale, (rows, rows))

    def hidden(s, e):
        group = planes[s] * 2 + flip(x, e)
        block = x_ref[pl.ds(pl.multiple_of(group * rows, rows), rows), :]
        for m in range(members):
            both = jnp.dot(block, w_ref[m], preferred_element_type=jnp.float32)
            gate, up = both[:, :units], both[:, units:]
            scale = jnp.concatenate([scale_ref[s, e, m]] * (units // rows), axis=1)
            hid_ref[s, e * rows:(e + 1) * rows, m * units:(m + 1) * units] = (
                jax.nn.silu(gate) * up * scale).astype(hid_ref.dtype)

    def down(s, g, es=(0, 1)):
        at_rows = pl.ds(es[0] * rows, len(es) * rows)

        @pl.loop(0, 2, unroll=True)
        def _(f):
            member = (y + f - 2 * y * f) * 2 + flip(c, g)
            at = pl.ds(pl.multiple_of(member * cols, cols), cols)
            part_ref[s, f, g, at_rows, :] = jnp.dot(
                hid_ref[s, at_rows, :], down_ref[:, at], preferred_element_type=jnp.float32).astype(part_ref.dtype)

    spans = spans_of(rows)
    tail = rows - spans[1][0] - spans[1][1]

    def x_first(h, s):
        return (h + s) % 2 == 1

    def local(h, a, b, s, g):
        e, f = (a, b) if x_first(h, s) else (b, a)
        return part_ref.at[s, f, g, pl.ds(e * rows + spans[h][0], spans[h][1]), :]

    def local_late(e, f, s, g):
        return part_ref.at[s, f, g, pl.ds((e + 1) * rows - tail, tail), :]

    def piece_c(h, a, b, s):
        return buf_c.at[h, a, b, s, pl.ds(0, spans[h][1]), :]

    def piece_1(h, b, s):
        return buf_1.at[h, b, s, pl.ds(0, spans[h][1]), :]

    def piece_2(h, s):
        return buf_2.at[h, s, pl.ds(0, spans[h][1]), :]

    def piece_z(h, k):
        return buf_z.at[h, k, pl.ds(0, spans[h][1]), :]

    def swap(s, es=(0, 1)):
        there = moved(here, sizes, other)
        for a, b in ((1, 1), (1, 0), (0, 1), (0, 0)):
            for h in range(2):
                if (a if x_first(h, s) else b) in es:
                    push(local(h, a, b, s, 1), piece_c(h, a, b, s), recv_c.at[a, b, s], there)
        for e in es:
            for f in range(2):
                push(local_late(e, f, s, 1), late_c.at[s, e, f], recv_lc.at[s, es[0]], there)

    def add(dst, *srcs):
        chunk = 16

        @pl.loop(0, dst.shape[0] // chunk)
        def _(i):
            at = pl.ds(pl.multiple_of(i * chunk, chunk), chunk)
            total = srcs[0][at, :].astype(jnp.float32)
            for src in srcs[1:]:
                total = total + src[at, :].astype(jnp.float32)
            dst[at, :] = total.astype(dst.dtype)

    def step_first(s, b):
        arrive_rows(rows - tail, recv_c.at[1, b, s])
        for h in range(2):
            piece = piece_c(h, 1, b, s)
            add(piece, piece, local(h, 1, b, s, 0))
            push(piece, piece_1(h, b, s), recv_1.at[h, b, s], moved(here, sizes, axis[1 - x_first(h, s)]))

    def step_second(s):
        arrive_rows(rows - tail, recv_c.at[0, 1, s])
        for h in range(2):
            piece = piece_c(h, 0, 1, s)
            arrive(piece_1(h, 1, s), recv_1.at[h, 1, s])
            add(piece, piece, local(h, 0, 1, s, 0), piece_1(h, 1, s))
            push(piece, piece_2(h, s), recv_2.at[h, s], moved(here, sizes, axis[int(x_first(h, s))]))

    def step_last(s):
        arrive_rows(rows - tail, recv_c.at[0, 0, s])
        for h in range(2):
            piece = piece_c(h, 0, 0, s)
            arrive(piece_1(h, 0, s), recv_1.at[h, 0, s])
            arrive(piece_2(h, s), recv_2.at[h, s])
            srcs = (piece, local(h, 0, 0, s, 0), piece_1(h, 0, s), piece_2(h, s))
            for k in {0: (0, 2), 3: (1,)}.get(s, ()):
                arrive(piece_z(h, k), recv_z.at[h, k])
                srcs += (piece_z(h, k),)
            if s:
                add(piece, *srcs)
                push(piece, piece_z(h, s - 1), recv_z.at[h, s - 1], (across if s == 3 else pair, x, y, c))
            else:
                add(out_ref.at[pl.ds(*spans[h]), :], *srcs)

    def late_out(s, es=(0, 1)):
        more = {0: (0, 2), 3: (1,)}.get(s, ())
        arrive_rows(2 * len(es) * tail, recv_lc.at[s, es[0]])
        for k in more:
            if es[-1]:
                arrive_rows(4 * tail, recv_lz.at[k])
        for e in es:
            for f in range(2):
                piece = late_c.at[s, e, f]
                add(piece, piece, local_late(e, f, s, 0), *[late_zs.at[k, e, f] for k in more])
                if s:
                    push(piece, late_zs.at[s - 1, e, f], recv_lz.at[s - 1], (across if s == 3 else pair, x, y, c))

    ways = [(i, pl.ds(i * 16, 16)) for i in range(tail // 16)]

    def late_piece(i, a, b, at):
        e, f = (b, a) if i else (a, b)
        return late_c.at[0, e, f, at, :]

    def late_first():
        for b in (1, 0):
            for i, at in ways:
                push(late_piece(i, 1, b, at), late_1.at[i, b], recv_l1.at[i, b], moved(here, sizes, axis[i]))

    def late_next():
        for i, at in ways:
            piece = late_piece(i, 0, 1, at)
            arrive(late_1.at[i, 1], recv_l1.at[i, 1])
            add(piece, piece, late_1.at[i, 1])
            push(piece, late_2.at[i], recv_l2.at[i], moved(here, sizes, axis[1 - i]))

    def late_last():
        for i, at in ways:
            arrive(late_1.at[i, 0], recv_l1.at[i, 0])
            arrive(late_2.at[i], recv_l2.at[i])
            add(out_ref.at[pl.ds(rows - tail + i * 16, 16), :], late_piece(i, 0, 0, at), late_1.at[i, 0], late_2.at[i])

    keep = pltpu.make_async_copy(own_share, share_ref.at[me], load_sem.at[3 + 3 * members])

    def send_shares():
        for rel in ep_rels:
            pltpu.make_async_remote_copy(
                src_ref=own_share, dst_ref=share_ref.at[me], send_sem=send_sem.at[1], recv_sem=share_recv,
                device_id=device(moved(here, sizes, rel)), device_id_type=MESH).start()
        keep.start()

    def wait_loads():
        for load in loads:
            load.wait()
        keep.wait()
        others = share_ref.at[pl.ds(0, len(ep_rels))]
        pltpu.make_async_copy(others, others, share_recv).wait()
        for s in range(nz):
            spread(s)

    start_z()
    start_late()
    pass_on(0)
    send_shares()
    late_second()
    relay(0, 1, 3)
    relay(1, 1, 3)
    pass_second(0)
    relay(2, 1, 3)
    meet(1)
    pass_on(1)
    relay(0, 2)
    wait_loads()
    relay(1, 2)
    relay(2, 2)
    late_z()
    pass_last(0)
    meet(2)
    pass_on(2)
    pass_second(1)
    whole(0)
    hidden(0, 0)
    hidden(0, 1)
    pass_second(2)
    meet(3)
    pass_on(3)
    late_relay(1)
    late_relay(3)
    down(0, 1)
    swap(0)
    down(0, 0)
    pass_last(1)
    late_meet(1)
    whole(1)
    hidden(1, 0)
    late_relay(2)
    pass_last(2)
    hidden(1, 1)
    pass_second(3)
    step_first(0, 1)
    late_meet(2)
    down(1, 1)
    swap(1)
    down(1, 0)
    whole(2)
    hidden(2, 1)
    step_first(1, 1)
    step_first(1, 0)
    hidden(2, 0)
    late_meet(3)
    pass_last(3)
    down(2, 1)
    swap(2)
    late_out(1)
    down(2, 0)
    step_first(2, 1)
    step_first(2, 0)
    late_out(2)
    whole(3)
    hidden(3, 1)
    down(3, 1, (1,))
    swap(3, (1,))
    down(3, 0, (1,))
    hidden(3, 0)
    step_second(2)
    step_first(3, 1)
    late_out(3, (1,))
    down(3, 1, (0,))
    swap(3, (0,))
    down(3, 0, (0,))
    step_first(3, 0)
    late_out(3, (0,))
    step_last(2)
    step_second(3)
    step_second(1)
    step_first(0, 0)
    step_second(0)
    step_last(3)
    late_out(0)
    late_first()
    step_last(1)
    late_next()
    step_last(0)
    late_last()
    for i, count in enumerate(sends):
        arrive_rows(count, send_sem.at[2 + i])
    gone = share_ref.at[pl.ds(0, len(ep_rels))]
    pltpu.make_async_copy(gone, gone, send_sem.at[1]).wait()

    @pl.when(is_inner)
    def _():
        arrive_rows(sum(relays), send_sem.at[0])


def cuts_of(rows):
    late = 32
    most = 48
    return [(0, most), (most, rows - late - most)] + ([(rows - late, late)] if late else [])


def strips_of(cuts):
    (_, a), (start, b) = cuts[:2]
    return [(0, a // 32 * 16), (a // 32 * 16, a - a // 32 * 16), (start, b)]


def spans_of(rows):
    late = 16
    most = (rows - late + 16) // 32 * 16
    return [(0, most), (most, rows - late - most)]


def layer_scratch(sizes, x, ids, prob, gate, down):
    nz = sizes[0]
    groups, parts = nz * sizes[1], sizes[2] * sizes[3]
    rows, cols = x.shape
    spans = spans_of(rows)
    half, tail = spans[0][1], rows - spans[1][0] - spans[1][1]
    members, width, units = gate.shape
    experts = groups * members
    buffers = [
        pltpu.VMEM((groups * rows, parts * cols), x.dtype),
        pltpu.VMEM(ids.shape, ids.dtype),
        pltpu.VMEM(prob.shape, prob.dtype),
        pltpu.VMEM((experts, rows), prob.dtype),
        pltpu.VMEM((groups, experts, rows), prob.dtype),
        pltpu.VMEM((members, width, 2 * units), gate.dtype),
        pltpu.VMEM((members * units, parts * cols), down.dtype),
        pltpu.VMEM((nz, 2 * rows, members * units), x.dtype),
        pltpu.VMEM((nz, 2, 2, 2 * rows, cols), x.dtype),
        pltpu.VMEM((2, 2, 2, nz, half, cols), x.dtype),
        pltpu.VMEM((2, 2, nz, half, cols), x.dtype),
        pltpu.VMEM((2, nz, half, cols), x.dtype),
        pltpu.VMEM((2, nz - 1, half, cols), x.dtype),
        pltpu.VMEM((nz, 2, 2, tail, cols), x.dtype),
        pltpu.VMEM((nz - 1, 2, 2, tail, cols), x.dtype),
        pltpu.VMEM((tail // 16, 2, 16, cols), x.dtype),
        pltpu.VMEM((tail // 16, 16, cols), x.dtype),
        pltpu.VMEM((nz, 2, members, rows, rows), jnp.float32),
    ]
    semaphores = [pltpu.SemaphoreType.DMA(shape) for shape in (
        (4 + 3 * members,), (12,), (3, 3 * nz), (3, nz), (nz,), (nz,), (), (2, 2, nz), (2, 2, nz), (2, nz), (2, nz - 1),
        (nz, 2), (nz - 1,), (tail // 16, 2), (tail // 16,))]
    return buffers, semaphores


def layer(sizes, x, ids, prob, gate, up, down):
    buffers, semaphores = layer_scratch(sizes, x, ids, prob, gate, down)
    return pl.pallas_call(
        functools.partial(layer_kernel, sizes),
        out_shape=jax.ShapeDtypeStruct(x.shape, x.dtype),
        in_specs=[pl.BlockSpec(memory_space=pl.ANY)] * 6,
        out_specs=pl.BlockSpec(memory_space=pltpu.VMEM),
        scratch_shapes=buffers + semaphores,
        compiler_params=pltpu.CompilerParams(collective_id=0, has_side_effects=True, vmem_limit_bytes=60 << 20),
        name="layer",
    )(x, ids, prob, gate, up, down)


def hidden_kernel(x_ref, w_ref, gate_ref, up_ref, out_ref):
    gate = jnp.dot(x_ref[...], gate_ref[0], preferred_element_type=jnp.float32)
    up = jnp.dot(x_ref[...], up_ref[0], preferred_element_type=jnp.float32)
    out_ref[...] = (jax.nn.silu(gate) * up * w_ref[0]).astype(out_ref.dtype)


def down_kernel(h_ref, down_ref, out_ref):
    out_ref[...] = jnp.dot(h_ref[...], down_ref[...], preferred_element_type=jnp.float32).astype(out_ref.dtype)


def tile_of(total, wanted):
    while total % wanted:
        wanted //= 2
    return wanted


def hidden_units(x, scale, gate_weight, up_weight):
    members, width, units = gate_weight.shape
    rows = x.shape[0]
    tile = tile_of(rows, 256)
    return pl.pallas_call(
        hidden_kernel,
        grid=(members, rows // tile),
        out_shape=jax.ShapeDtypeStruct((rows, members * units), x.dtype),
        in_specs=[
            pl.BlockSpec((tile, width), lambda e, m: (m, 0)),
            pl.BlockSpec((1, tile, 1), lambda e, m: (e, m, 0)),
            pl.BlockSpec((1, width, units), lambda e, m: (e, 0, 0)),
            pl.BlockSpec((1, width, units), lambda e, m: (e, 0, 0)),
        ],
        out_specs=pl.BlockSpec((tile, units), lambda e, m: (m, e)),
        compiler_params=pltpu.CompilerParams(vmem_limit_bytes=40 << 20),
        name="hidden",
    )(x, scale, gate_weight, up_weight)


def down_product(hidden, down_weight):
    members, units, width = down_weight.shape
    rows = hidden.shape[0]
    down = down_weight.reshape(members * units, width)
    tile_n = tile_of(width, 512)
    tile_m = tile_of(rows, 1024)
    return pl.pallas_call(
        down_kernel,
        grid=(rows // tile_m, width // tile_n),
        out_shape=jax.ShapeDtypeStruct((rows, width), hidden.dtype),
        in_specs=[
            pl.BlockSpec((tile_m, members * units), lambda m, n: (m, 0)),
            pl.BlockSpec((members * units, tile_n), lambda m, n: (0, n)),
        ],
        out_specs=pl.BlockSpec((tile_m, tile_n), lambda m, n: (m, n)),
        compiler_params=pltpu.CompilerParams(vmem_limit_bytes=50 << 20),
        name="down",
    )(hidden, down)


def body(tokens, expert_ids, gate_prob, gate_weight, up_weight, down_weight):
    groups, parts = lax.axis_size("ep"), lax.axis_size("etp")
    members = gate_weight.shape[0]
    sizes = (groups // 2, 2, parts // 2, 2)
    rows = tokens.shape[0]
    square = groups == 8 and parts == 4 and members * groups <= rows == 128
    if square:
        ids, prob = jnp.transpose(expert_ids), jnp.transpose(gate_prob)
        buffers = layer_scratch(sizes, tokens, ids, prob, gate_weight, down_weight)[0]
        size = sum(math.prod(b.shape) * b.dtype.itemsize for b in buffers)
        if size <= VMEM_BUDGET:
            return layer(sizes, tokens, ids, prob, gate_weight, up_weight, down_weight)
    numbers = jnp.arange(members * groups, dtype=jnp.int32)
    share = jnp.sum(jnp.where(expert_ids[:, :, None] == numbers, gate_prob[:, :, None], 0.0), axis=1)
    gathered = lax.all_gather(lax.all_gather(tokens, "ep", axis=0, tiled=True), "etp", axis=1, tiled=True)
    shares = lax.all_gather(share, "ep", axis=0, tiled=True)
    mine = lax.dynamic_slice_in_dim(shares, lax.axis_index("ep") * members, members, axis=1)
    hidden = hidden_units(gathered, jnp.transpose(mine)[:, :, None], gate_weight, up_weight)
    partial_sum = down_product(hidden, down_weight)
    summed = lax.psum_scatter(partial_sum, "etp", scatter_dimension=1, tiled=True)
    return lax.psum_scatter(summed, "ep", scatter_dimension=0, tiled=True)


def solution(mesh):
    in_specs = (
        P("ep", "etp"),
        P("ep", None),
        P("ep", None),
        P("ep", None, "etp"),
        P("ep", None, "etp"),
        P("ep", "etp", None),
    )
    out_specs = P("ep", "etp")
    return jax.shard_map(body, mesh=mesh, in_specs=in_specs, out_specs=out_specs, check_vma=False)
```
